256 devices in a mesh: gx: 16 (over z, core), gy: 4 (over y), ma: 4 (over x).
Axes of the slice: x: 4, y: 4, z: 8, core: 2. Of those that a mesh axis runs over, the one named last changes fastest.
Arguments:
- object_field: float32 [2, 2048, 1024], P(None, 'gx', 'gy'), may hold values from -5 to 5
- probe_modes: float32 [8, 2, 256, 256], P('ma'), may hold values from -1.5 to 1.5
- measured: float32 [16, 4, 2, 256, 256], P('gx', 'gy'), may hold values from 0.1 to 4
- positions: int32 [16, 4, 2, 2], P('gx', 'gy'), may hold values from 0 to 255, as said below
- slot_counts: int32 [16, 4], P('gx', 'gy'), may hold values from 1 to 2, as said below
Outputs:
- updated_object: float32 [2, 2048, 1024], P(None, 'gx', 'gy')
The draws below stay inside these ranges and needn't reach their ends.
Inputs may be any that keep to these rules, and one draw needn't show every extreme that they name: positions[a, b, s] holds a row 0 to 127 and a column 0 to 255 of tile (a, b); slots s >= slot_counts[a, b] are unused. `slot_counts`: some tile uses all 2 slots.
All inputs are finite; a program needn't handle non-finite values.
Results may differ from the reference program's by a relative error of at most 0.0023.
Values sent between devices are 32-bit elements; how exact they have to be, the bound alone decides.
A program may use at most 64 MiB of HBM per device.

```python
import math
import jax
import jax.numpy as jnp
from jax import lax

PATCH = 256
MODES = 8
TX = 128
TY = 256
CAP = 2
OUTER = 2
ITERS = 1
GRID_X = 16
GRID_Y = 4
NX = 2048
NY = 1024


def draw_positions(key, part):
    row_draw = jax.random.randint(jax.random.fold_in(key, 11), (GRID_X, GRID_Y, CAP, 1), 0, TX, dtype=jnp.int32)
    col_draw = jax.random.randint(jax.random.fold_in(key, 12), (GRID_X, GRID_Y, CAP, 1), 0, TY, dtype=jnp.int32)
    return jnp.concatenate([row_draw, col_draw], -1).astype(jnp.int32)


def draw_slot_counts(key, part):
    base_counts = jax.random.randint(jax.random.fold_in(key, 21), (GRID_X, GRID_Y), 1, CAP + 1, dtype=jnp.int32)
    chosen = jax.random.randint(jax.random.fold_in(key, 22), (), 0, GRID_X * GRID_Y, dtype=jnp.int32)
    tile_ids = jnp.arange(GRID_X * GRID_Y, dtype=jnp.int32).reshape(GRID_X, GRID_Y)
    return jnp.where(tile_ids == chosen, CAP, base_counts).astype(jnp.int32)


def level_of(key, shape, pieces, least, top_value):
    gain, own = 1.0, jax.random.fold_in(key, 6)
    for dim, blocks in pieces:
        heights = jnp.exp(jax.random.uniform(jax.random.fold_in(own, dim), (blocks,), jnp.float32, least / len(pieces), top_value / len(pieces)))
        gain = gain * jnp.repeat(heights, shape[dim] // blocks).reshape([-1 if axis == dim else 1 for axis in range(len(shape))])
    return gain


def noise(stream_key, extent, deviation, reach, pieces=(), kind=jnp.bfloat16):
    values = jax.random.normal(stream_key, extent, jnp.float32) * deviation
    if len(pieces) > 0:
        values = level_of(stream_key, extent, pieces, -0.22, 0.18) * values
    return jnp.clip(values, min=-reach, max=reach).astype(kind)


def setup_inputs(seed: int = 0) -> dict:
    streams_of = jax.random.split(jax.random.key(seed), 6)
    object_field = noise(streams_of[0], (2, NX, NY), 0.7, 5.0, ((1, 16), (2, 4)), jnp.float32)
    probe_modes = noise(streams_of[1], (MODES, 2, PATCH, PATCH), 0.25, 1.5, ((0, 4),), jnp.float32)
    measured = jnp.clip(jnp.exp(math.log(4.0) - 3.6888794 * jax.random.uniform(streams_of[2], (GRID_X, GRID_Y, CAP, PATCH, PATCH), jnp.float32) ** level_of(streams_of[2], (GRID_X, GRID_Y, CAP, PATCH, PATCH), ((0, 16), (1, 4)), -0.2, 0.2)), 0.1, 4.0)
    positions = draw_positions(jax.random.fold_in(streams_of[5], 71), 0)
    slot_counts = draw_slot_counts(jax.random.fold_in(streams_of[5], 71), 0)
    return {"object_field": object_field, "probe_modes": probe_modes, "measured": measured, "positions": positions, "slot_counts": slot_counts}


DAMPING = 1.0

def dft_tables(patch_width):
    ladder = jnp.arange(patch_width, dtype=jnp.int32)
    phases = ladder[:, None] * ladder[None, :] % patch_width
    angles = phases.astype(jnp.float32) * (2.0 * math.pi / patch_width)
    factor = 1.0 / math.sqrt(patch_width)
    real_part = jnp.cos(angles) * factor
    imag_part = -jnp.sin(angles) * factor
    table_one = jnp.concatenate([jnp.concatenate([real_part, -imag_part], 1), jnp.concatenate([imag_part, real_part], 1)], 0).astype(jnp.bfloat16)
    table_two = jnp.concatenate([jnp.concatenate([real_part, imag_part], 1), jnp.concatenate([-imag_part, real_part], 1)], 0).astype(jnp.bfloat16)
    return (table_one, table_two)

def forward_ref(wavefield, tables):
    patch_width = wavefield.shape[-1]
    first_table = tables[0].astype(jnp.float32).reshape(2, patch_width, 2, patch_width)
    second_table = tables[1].astype(jnp.float32).reshape(2, patch_width, 2 * patch_width)
    halfway = jnp.einsum('pqci,bcik->bpqk', first_table, wavefield.astype(jnp.float32)).astype(jnp.bfloat16)
    halfway = lax.optimization_barrier(halfway)
    return jnp.einsum('bcik,ckl->bil', halfway.astype(jnp.float32), second_table)

def adjoint_ref(weighted, tables):
    patch_width = weighted.shape[1]
    halfway = jnp.einsum('bik,kl->bil', weighted.astype(jnp.float32), tables[0].astype(jnp.float32)).astype(jnp.bfloat16)
    halfway = lax.optimization_barrier(halfway)
    second_table = tables[1].astype(jnp.float32).reshape(2, patch_width, 2, patch_width)
    return jnp.einsum('pqci,bicl->bpql', second_table, halfway.astype(jnp.float32).reshape(halfway.shape[0], patch_width, 2, patch_width))

def exit_waves(probe_modes, windows):
    probe_real = probe_modes[None, :, 0]
    probe_imag = probe_modes[None, :, 1]
    window_real = windows[:, None, 0]
    window_imag = windows[:, None, 1]
    real_part = probe_real * window_real - probe_imag * window_imag
    imag_part = probe_real * window_imag + probe_imag * window_real
    wavefield = jnp.stack([real_part, imag_part], 2).astype(jnp.bfloat16)
    wavefield = lax.optimization_barrier(wavefield)
    return wavefield.reshape(-1, 2, probe_modes.shape[-1], probe_modes.shape[-1])

def intensity_part(spectra, mode_count):
    patch_width = spectra.shape[1]
    grouped = spectra.reshape(-1, mode_count, patch_width, 2 * patch_width)
    squared = grouped * grouped
    return lax.optimization_barrier(jnp.sum(squared[..., :patch_width] + squared[..., patch_width:], axis=1))

def change_part(spectra, moved_spectra, mode_count):
    patch_width = spectra.shape[1]
    grouped = spectra.reshape(-1, mode_count, patch_width, 2 * patch_width)
    shifted = moved_spectra.reshape(-1, mode_count, patch_width, 2 * patch_width)
    product = grouped * shifted
    return 2.0 * lax.optimization_barrier(jnp.sum(product[..., :patch_width] + product[..., patch_width:], axis=1))

def mode_images(weights, spectra, probe_modes, tables):
    mode_count = probe_modes.shape[0]
    patch_width = probe_modes.shape[-1]
    doubled = jnp.concatenate([weights, weights], -1)
    grouped = spectra.reshape(-1, mode_count, patch_width, 2 * patch_width)
    weighted = (2.0 * grouped * doubled[:, None]).astype(jnp.bfloat16)
    weighted = lax.optimization_barrier(weighted)
    returned = adjoint_ref(weighted.reshape(-1, patch_width, 2 * patch_width), tables)
    returned = returned.reshape(-1, mode_count, 2, patch_width, patch_width)
    probe_real = probe_modes[None, :, 0]
    probe_imag = probe_modes[None, :, 1]
    real_part = lax.optimization_barrier(jnp.sum(probe_real * returned[:, :, 0] + probe_imag * returned[:, :, 1], axis=1))
    imag_part = lax.optimization_barrier(jnp.sum(probe_real * returned[:, :, 1] - probe_imag * returned[:, :, 0], axis=1))
    return jnp.stack([real_part, imag_part], 1)

def reference(object_field, probe_modes, measured, positions, slot_counts):
    half_width = PATCH // 2
    tables = dft_tables(PATCH)
    first_rows = (jnp.arange(GRID_X, dtype=jnp.int32) * TX)[:, None, None]
    first_cols = (jnp.arange(GRID_Y, dtype=jnp.int32) * TY)[None, :, None]
    corner_rows = (positions[..., 0] + first_rows).reshape(-1).astype(jnp.int32)
    corner_cols = (positions[..., 1] + first_cols).reshape(-1).astype(jnp.int32)
    corners = jnp.stack([corner_rows, corner_cols], 1)
    live_mask = (jnp.arange(CAP, dtype=jnp.int32)[None, None, :] < slot_counts[:, :, None]).astype(jnp.float32).reshape(-1)[:, None, None]
    targets = measured.reshape(-1, PATCH, PATCH)
    anchor = jnp.zeros((), jnp.int32)

    def padded_of(current):
        return jnp.pad(current, ((0, 0), (half_width, half_width), (half_width, half_width)))

    def spectra_of(current):
        padded = padded_of(current)

        def one_pattern(corner):
            window = lax.dynamic_slice(padded, (anchor, corner[0], corner[1]), (2, PATCH, PATCH))
            return forward_ref(exit_waves(probe_modes, window[None]), tables)
        return lax.map(one_pattern, corners)

    def project(weights, spectra):
        canvas = jnp.zeros((2, NX + PATCH, NY + PATCH), jnp.float32)

        def place(canvas, inputs):
            corner, weight, spectrum = inputs
            piece = mode_images(weight[None], spectrum, probe_modes, tables)[0]
            where = (anchor, corner[0], corner[1])
            canvas = lax.dynamic_update_slice(canvas, lax.dynamic_slice(canvas, where, (2, PATCH, PATCH)) + piece, where)
            return (canvas, None)
        canvas = lax.scan(place, canvas, (corners, weights, spectra))[0]
        return canvas[:, half_width:half_width + NX, half_width:half_width + NY]
    current = object_field
    for outer_step in range(OUTER):
        spectra = spectra_of(current)

        def one_intensity(spectrum):
            return intensity_part(spectrum, MODES)[0]
        intensity = lax.map(one_intensity, spectra)
        misfit = live_mask * (intensity - targets)
        gradient = project(misfit, spectra)

        def operator(vector):
            padded = padded_of(vector)

            def one_change(inputs):
                corner, spectrum = inputs
                window = lax.dynamic_slice(padded, (anchor, corner[0], corner[1]), (2, PATCH, PATCH))
                moved_spectra = forward_ref(exit_waves(probe_modes, window[None]), tables)
                return change_part(spectrum, moved_spectra, MODES)[0]
            change = live_mask * lax.map(one_change, (corners, spectra))
            return project(change, spectra) + DAMPING * vector
        update = jnp.zeros_like(current)
        residual = -gradient
        direction = residual
        norm_now = jnp.sum(residual * residual)
        for inner_step in range(ITERS):
            applied = operator(direction)
            step_size = norm_now / jnp.sum(direction * applied)
            update = update + step_size * direction
            residual = residual - step_size * applied
            if inner_step + 1 < ITERS:
                norm_next = jnp.sum(residual * residual)
                direction = residual + norm_next / norm_now * direction
                norm_now = norm_next
        current = current + update
    return current
```

```python
import math

import jax
import jax.numpy as jnp
from jax import lax
from jax.sharding import Mesh
from jax.sharding import PartitionSpec as P

OUTER = 2
GX = ("gx_0", "gx_1")
GX_GY = ("gx_0", "gx_1", "gy")


DAMPING = 1.0


def padded_2(block, sides, width):
    for axis, dim in sides:
        count = lax.axis_size(axis)
        forward = [(i, i + 1) for i in range(count - 1)]
        backward = [(target, source) for source, target in forward]
        low = lax.ppermute(
            lax.slice_in_dim(block, block.shape[dim] - width, None, axis=dim), axis, forward
        )
        high = lax.ppermute(lax.slice_in_dim(block, 0, width, axis=dim), axis, backward)
        block = jnp.concatenate([low, block, high], axis=dim)
    return block


def from_everyone(value, axis):
    copies = jnp.broadcast_to(value, (lax.axis_size(axis), *value.shape))
    return lax.all_to_all(copies, axis, split_axis=0, concat_axis=0, tiled=True)


def taken_together(value, axis):
    return from_everyone(value, axis).sum(axis=0)


def cut_along(value, dim, count):
    before, after = (value.shape[:dim], value.shape[dim + 1 :])
    return jnp.moveaxis(value.reshape(*before, count, -1, *after), dim, 0)


def summed_on_arrival(value, axis, dim):
    count = lax.axis_size(axis)
    blocks = lax.all_to_all(cut_along(value, dim, count), axis, 0, 0, tiled=True)
    return jnp.sum(blocks, axis=0)


def joined_along(blocks, dim):
    lengths = list(blocks.shape[1:])
    lengths[dim] *= blocks.shape[0]
    return jnp.moveaxis(blocks, 0, dim).reshape(lengths)


def gather_directly(value, axis, dim):
    return joined_along(from_everyone(value, axis), dim)


def dft_tables(patch_width):
    ladder = jnp.arange(patch_width, dtype=jnp.int32)
    phases = ladder[:, None] * ladder[None, :] % patch_width
    angles = phases.astype(jnp.float32) * (2.0 * math.pi / patch_width)
    factor = 1.0 / math.sqrt(patch_width)
    real_part = jnp.cos(angles) * factor
    imag_part = -jnp.sin(angles) * factor
    table_one = jnp.concatenate(
        [jnp.concatenate([real_part, -imag_part], 1), jnp.concatenate([imag_part, real_part], 1)], 0
    ).astype(jnp.bfloat16)
    table_two = jnp.concatenate(
        [jnp.concatenate([real_part, imag_part], 1), jnp.concatenate([-imag_part, real_part], 1)], 0
    ).astype(jnp.bfloat16)
    return (table_one, table_two)


def forward_transform(wavefield, tables):
    patch_width = wavefield.shape[-1]
    halfway = jnp.einsum(
        "pqci,bcik->bpqk",
        tables[0].reshape(2, patch_width, 2, patch_width),
        wavefield,
        preferred_element_type=jnp.float32,
    ).astype(jnp.bfloat16)
    return jnp.einsum(
        "bcik,ckl->bil",
        halfway,
        tables[1].reshape(2, patch_width, 2 * patch_width),
        preferred_element_type=jnp.float32,
    )


def adjoint_transform(weighted, tables):
    patch_width = weighted.shape[1]
    halfway = jnp.einsum(
        "bik,kl->bil", weighted, tables[0], preferred_element_type=jnp.float32
    ).astype(jnp.bfloat16)
    return jnp.einsum(
        "pqci,bicl->bpql",
        tables[1].reshape(2, patch_width, 2, patch_width),
        halfway.reshape(halfway.shape[0], patch_width, 2, patch_width),
        preferred_element_type=jnp.float32,
    )


def exit_waves(probe_modes, windows):
    probe_real = probe_modes[None, :, 0]
    probe_imag = probe_modes[None, :, 1]
    window_real = windows[:, None, 0]
    window_imag = windows[:, None, 1]
    real_part = probe_real * window_real - probe_imag * window_imag
    imag_part = probe_real * window_imag + probe_imag * window_real
    wavefield = jnp.stack([real_part, imag_part], 2).astype(jnp.bfloat16)
    return wavefield.reshape(-1, 2, probe_modes.shape[-1], probe_modes.shape[-1])


def intensity_part(spectra, mode_count):
    patch_width = spectra.shape[1]
    grouped = spectra.reshape(-1, mode_count, patch_width, 2 * patch_width)
    squared = grouped * grouped
    return jnp.sum(squared[..., :patch_width] + squared[..., patch_width:], axis=1)


def change_part(spectra, moved_spectra, mode_count):
    patch_width = spectra.shape[1]
    grouped = spectra.reshape(-1, mode_count, patch_width, 2 * patch_width)
    shifted = moved_spectra.reshape(-1, mode_count, patch_width, 2 * patch_width)
    product = grouped * shifted
    return 2.0 * jnp.sum(product[..., :patch_width] + product[..., patch_width:], axis=1)


def mode_images(weights, spectra, probe_modes, tables):
    mode_count = probe_modes.shape[0]
    patch_width = probe_modes.shape[-1]
    doubled = jnp.concatenate([weights, weights], -1)
    grouped = spectra.reshape(-1, mode_count, patch_width, 2 * patch_width)
    weighted = (2.0 * grouped * doubled[:, None]).astype(jnp.bfloat16)
    returned = adjoint_transform(weighted.reshape(-1, patch_width, 2 * patch_width), tables)
    returned = returned.reshape(-1, mode_count, 2, patch_width, patch_width)
    probe_real = probe_modes[None, :, 0]
    probe_imag = probe_modes[None, :, 1]
    real_part = jnp.sum(probe_real * returned[:, :, 0] + probe_imag * returned[:, :, 1], axis=1)
    imag_part = jnp.sum(probe_real * returned[:, :, 1] - probe_imag * returned[:, :, 0], axis=1)
    return jnp.stack([real_part, imag_part], 1)


def fold_edges(widened, axis_dim, length, rim_width):
    middle = lax.slice_in_dim(widened, 2 * rim_width, 2 * rim_width + length, axis=axis_dim)
    low_rim = lax.slice_in_dim(widened, 0, rim_width, axis=axis_dim)
    high_rim = lax.slice_in_dim(
        widened, length + 3 * rim_width, length + 4 * rim_width, axis=axis_dim
    )
    low_pads = [(0, 0), (0, 0), (0, 0)]
    high_pads = [(0, 0), (0, 0), (0, 0)]
    low_pads[axis_dim] = (0, length - rim_width)
    high_pads[axis_dim] = (length - rim_width, 0)
    return middle + jnp.pad(low_rim, low_pads) + jnp.pad(high_rim, high_pads)


def shards(object_field, probe_modes, measured, positions, slot_counts):
    patch_width = probe_modes.shape[-1]
    mode_count = probe_modes.shape[0]
    rim_width = patch_width // 2
    tile_rows = object_field.shape[1]
    tile_cols = object_field.shape[2]
    slot_count = measured.shape[2]
    tables = dft_tables(patch_width)
    targets = measured[0, 0]
    centres = positions[0, 0]
    live_mask = (jnp.arange(slot_count, dtype=jnp.int32) < slot_counts[0, 0]).astype(jnp.float32)[
        :, None, None
    ]
    anchor = jnp.zeros((), jnp.int32)

    def spectra_of(current):
        padded = padded_2(current, ((GX, 1), ("gy", 2)), rim_width)
        windows = jnp.stack(
            [
                lax.dynamic_slice(
                    padded,
                    (anchor, centres[slot_index, 0], centres[slot_index, 1]),
                    (2, patch_width, patch_width),
                )
                for slot_index in range(slot_count)
            ],
            0,
        )
        return forward_transform(exit_waves(probe_modes, windows), tables)

    def mode_total(partial_value):
        return taken_together(partial_value, "ma")

    def combine(folded):
        summed = summed_on_arrival(folded, "ma", 1)
        return summed

    def project(weights, spectra):
        pieces = mode_images(weights, spectra, probe_modes, tables)
        extended = jnp.zeros((2, tile_rows + patch_width, tile_cols + patch_width), jnp.float32)
        for slot_index in range(slot_count):
            corner = (anchor, centres[slot_index, 0], centres[slot_index, 1])
            extended = lax.dynamic_update_slice(
                extended,
                lax.dynamic_slice(extended, corner, (2, patch_width, patch_width))
                + pieces[slot_index],
                corner,
            )
        widened = padded_2(extended, ((GX, 1), ("gy", 2)), rim_width)
        folded = fold_edges(fold_edges(widened, 1, tile_rows, rim_width), 2, tile_cols, rim_width)
        result = combine(folded)
        return result

    def to_whole(vector):
        whole = gather_directly(vector, "ma", 1)
        return whole

    current = object_field
    spectra = spectra_of(current)
    intensity = mode_total(intensity_part(spectra, mode_count))
    for outer_step in range(OUTER):
        misfit = live_mask * (intensity - targets)
        direction = to_whole(-project(misfit, spectra))
        moved_spectra = spectra_of(direction)
        raw_change = mode_total(change_part(spectra, moved_spectra, mode_count))
        change = live_mask * raw_change
        norm_now = jnp.sum(direction * direction)
        totals = lax.psum(jnp.stack([norm_now, jnp.sum(change * change)]), GX_GY)
        step_size = totals[0] / (totals[1] + DAMPING * totals[0])
        current = current + step_size * direction
        if outer_step + 1 < OUTER:
            moved_intensity = mode_total(intensity_part(moved_spectra, mode_count))
            intensity = intensity + step_size * (raw_change + step_size * moved_intensity)
            spectra = spectra + step_size * moved_spectra
    return current


def solution(mesh):
    finer = Mesh(
        mesh.devices.reshape(8, 2, mesh.shape["gy"], mesh.shape["ma"]), ("gx_0", "gx_1", "gy", "ma")
    )
    placed = (
        P(None, GX, "gy"),
        P("ma", None, None, None),
        P(GX, "gy", None, None, None),
        P(GX, "gy", None, None),
        P(GX, "gy"),
    )
    return jax.shard_map(
        shards, mesh=finer, in_specs=placed, out_specs=P(None, GX, "gy"), check_vma=False
    )
```

```python
import functools
import math

import jax
import jax.numpy as jnp
import numpy as np
from jax import lax
from jax.experimental import pallas as pl
from jax.experimental.pallas import tpu as pltpu
from jax.sharding import PartitionSpec as P

OUTER = 2
DAMPING = 1.0
MESH = pl.DeviceIdType.MESH
F32 = jnp.float32
BF16 = jnp.bfloat16


def dft_parts(n):
    ladder = np.arange(n, dtype=np.int32)
    phases = ladder[:, None] * ladder[None, :] % n
    angles = phases.astype(np.float32) * np.float32(2.0 * math.pi / n)
    factor = np.float32(1.0 / math.sqrt(n))
    return np.stack([np.cos(angles) * factor, -np.sin(angles) * factor]).astype(BF16)


class Copies:
    def __init__(self, send_sems, recv_sems):
        self.send_sems, self.recv_sems, self.count, self.pending = send_sems, recv_sems, 0, []

    def make(self, src, dst, device, sends=None):
        copy = pltpu.make_async_remote_copy(
            src_ref=src,
            dst_ref=dst,
            send_sem=self.send_sems.at[self.count],
            recv_sem=self.recv_sems.at[self.count],
            device_id=device,
            device_id_type=MESH,
        )
        self.count += 1
        self.pending.append((copy, sends))
        return copy

    def finish(self):
        for copy, sends in self.pending:
            when(sends, copy.wait_send)
        self.pending = []


def when(condition, action):
    if condition is None:
        action()
    else:
        pl.when(condition)(action)


def kernel(
    dims,
    obj_hbm,
    probe_hbm,
    meas_hbm,
    pos_ref,
    count_ref,
    w_ref,
    out_ref,
    obj,
    cur,
    probes,
    meas,
    t_one,
    t_two,
    t_back,
    t_three,
    win,
    wave,
    half,
    spec,
    moved,
    turned,
    weight,
    placed,
    cut_rows,
    cut_cols,
    put_rows,
    put_cols,
    terms_a,
    terms_b,
    terms_c,
    terms_d,
    ext,
    dirs,
    from_z,
    from_y,
    from_ma,
    sums_ma,
    sums_gy,
    sums_gx,
    local_sems,
    send_sems,
    recv_sems,
):
    n_gx, n_gy, n_ma, n, tx, ty = dims
    rim = n // 2
    kh = n // 2
    gx, gy, ma = lax.axis_index("gx"), lax.axis_index("gy"), lax.axis_index("ma")
    core = lax.rem(gx, 2)
    slot, part_k = ma // 2, lax.rem(ma, 2)
    up, down = gx > 0, gx < n_gx - 1
    left, right = gy > 0, gy < n_gy - 1
    copies = Copies(send_sems, recv_sems)
    terms = (terms_a, terms_b, terms_c, terms_d)

    barrier = pltpu.get_barrier_semaphore()
    for axis, size, me in (("gx", n_gx, gx), ("gy", n_gy, gy), ("ma", n_ma, ma)):
        for o in range(1, size):
            pl.semaphore_signal(
                barrier, inc=1, device_id={axis: lax.rem(me + o, size)}, device_id_type=MESH
            )

    k_rows = pl.ds(pl.multiple_of(part_k * kh, kh), kh)
    own_rows, own_cols = pl.ds(rim, tx), pl.ds(rim, ty)
    loads = [
        pltpu.make_async_copy(obj_hbm, cur.at[:, own_rows, own_cols], local_sems.at[0]),
        pltpu.make_async_copy(obj_hbm, obj, local_sems.at[1]),
        pltpu.make_async_copy(probe_hbm, probes.at[0], local_sems.at[2]),
        pltpu.make_async_copy(meas_hbm.at[0, 0, slot, k_rows], meas, local_sems.at[3]),
    ]
    for load in loads:
        load.start()

    w_re, w_im = w_ref[0], w_ref[1]
    t_two[:n, :n], t_two[:n, n:], t_two[n:, :n], t_two[n:, n:] = w_re, w_im, -w_im, w_re
    t_back[:n, :n], t_back[:n, n:], t_back[n:, :n], t_back[n:, n:] = w_re, -w_im, w_im, w_re
    wk_re, wk_im = w_ref[0, k_rows, :], w_ref[1, k_rows, :]
    t_one[:kh, :n], t_one[:kh, n:], t_one[kh:, :n], t_one[kh:, n:] = wk_re, -wk_im, wk_im, wk_re
    k_cols = pl.ds(pl.multiple_of(part_k * kh, kh), kh)
    wc_re, wc_im = w_ref[0, :, k_cols], w_ref[1, :, k_cols]
    t_three[:n, :kh], t_three[:n, kh:] = wc_re, wc_im
    t_three[n:, :kh], t_three[n:, kh:] = -wc_im, wc_re

    def clear(ref):
        ref[...] = jnp.zeros(ref.shape, ref.dtype)

    padded = [cur] + [dirs.at[it] for it in range(OUTER)]
    for p in range(2):
        for buf in padded:
            when(gx == 0, functools.partial(clear, buf.at[p, pl.ds(0, rim)]))
            when(gx == n_gx - 1, functools.partial(clear, buf.at[p, pl.ds(rim + tx, rim)]))
            when(gy == 0, functools.partial(clear, buf.at[p, own_rows, pl.ds(0, rim)]))
            when(gy == n_gy - 1, functools.partial(clear, buf.at[p, own_rows, pl.ds(rim + ty, rim)]))
        for it in range(OUTER):
            when(gx == n_gx - 1, functools.partial(clear, from_z.at[it, 0, p]))
            when(gx == 0, functools.partial(clear, from_z.at[it, 1, p]))
            when(gy == n_gy - 1, functools.partial(clear, from_y.at[it, 0, p]))
            when(gy == 0, functools.partial(clear, from_y.at[it, 1, p]))

    for load in loads:
        load.wait()
    pl.semaphore_wait(barrier, n_gx + n_gy + n_ma - 3)

    ma_next, ma_prev = {"ma": lax.rem(ma + 1, n_ma)}, {"ma": lax.rem(ma + n_ma - 1, n_ma)}
    partner = {"gx": gx + 1 - 2 * core}
    ring = {}
    for part, other in ((0, 1), (1, 0)):
        ring["n", part] = copies.make(probes.at[0, core, part], probes.at[1, core, part], ma_next)
        ring["p", other] = copies.make(probes.at[0, core, other], probes.at[3, core, other], ma_prev)
        ring["n", part].start()
        ring["p", other].start()

    def shift_y(buf, p):
        low = copies.make(
            buf.at[p, own_rows, pl.ds(rim, rim)],
            buf.at[p, own_rows, pl.ds(rim + ty, rim)],
            {"gy": gy - 1},
            left,
        )
        high = copies.make(
            buf.at[p, own_rows, pl.ds(ty, rim)],
            buf.at[p, own_rows, pl.ds(0, rim)],
            {"gy": gy + 1},
            right,
        )
        when(left, low.start)
        when(right, high.start)
        return ((right, low), (left, high))

    def shift_x(buf, p):
        low = copies.make(
            buf.at[p, own_rows], buf.at[p, pl.ds(rim + tx, rim)], {"gx": gx - 1}, up
        )
        high = copies.make(buf.at[p, own_rows], buf.at[p, pl.ds(0, rim)], {"gx": gx + 1}, down)
        when(up, low.start)
        when(down, high.start)
        return ((down, low), (up, high))

    def arrive(arrivals):
        for condition, copy in arrivals:
            when(condition, copy.wait_recv)

    def widen(buf):
        beside = [shift_y(buf, p) for p in range(2)]
        return beside

    def widen_end(buf, beside):
        stacked = []
        for p in range(2):
            arrive(beside[p])
            stacked.append(shift_x(buf, p))
        for p in range(2):
            arrive(stacked[p])

    widen_end(cur, widen(cur))

    row_at, col_at = pos_ref[0, 0, slot, 0], pos_ref[0, 0, slot, 1]
    live = jnp.where(slot < count_ref[0, 0], 1.0, 0.0).astype(F32)
    tall, width = 2 * rim + tx, 2 * rim + ty

    def chosen(shape, dim, first):
        here = lax.broadcasted_iota(jnp.int32, shape, dim)
        there = lax.broadcasted_iota(jnp.int32, shape, 1 - dim)
        return jnp.where(here == there + first, 1.0, 0.0).astype(BF16)

    for i in range(2):
        cut_rows[:, i * tall : (i + 1) * tall] = chosen((n, tall), 1, row_at)
        cut_cols[i * width : (i + 1) * width] = chosen((width, n), 0, col_at)
        put_rows[:, i * n : (i + 1) * n] = chosen((tall, n), 0, row_at)
        put_cols[i * n : (i + 1) * n] = chosen((n, width), 1, col_at)

    def two_terms(x, ref, axis):
        top = x.astype(BF16)
        rest = (x - top.astype(F32)).astype(BF16)
        size = x.shape[axis]
        if axis == 0:
            ref[:size], ref[size:] = top, rest
        else:
            ref[:, :size], ref[:, size:] = top, rest
        return ref[...]

    def dot(x, y):
        return jnp.dot(x, y, preferred_element_type=F32)

    def window(buf):
        def cut(p, _):
            x = dot(two_terms(buf[p], terms[0], 1), cut_cols[...])
            win[p] = dot(cut_rows[...], two_terms(x, terms[1], 0))
            return 0

        lax.fori_loop(0, 2, cut, 0)

    def forward_pair(d):
        for c in range(2):
            pr, pi = probes[d, c, 0], probes[d, c, 1]
            wr, wi = win[0], win[1]
            wave[c, :n] = (pr * wr - pi * wi).astype(BF16)
            wave[c, n:] = (pr * wi + pi * wr).astype(BF16)
            h = dot(t_one[...], wave[c]).astype(BF16)
            half[c * kh : (c + 1) * kh, :n] = h[:kh]
            half[c * kh : (c + 1) * kh, n:] = h[kh:]
        return dot(half[...], t_two[...])

    def pair_rows(d):
        return pl.ds(pl.multiple_of(d * n, n), n)

    def folded(x):
        x = x[:kh] + x[kh:]
        return x[:, :n] + x[:, n:]

    def backward(misfit):
        weight[:, :n] = 2.0 * misfit
        weight[:, n:] = 2.0 * misfit

        def pair(d, _):
            y = weight[...]
            f = spec[pair_rows(d), :]
            half[:kh] = (f[:kh] * y).astype(BF16)
            half[kh:] = (f[kh:] * y).astype(BF16)
            b = dot(half[...], t_back[...]).astype(BF16)
            for c in range(2):
                turned[c, :kh] = b[c * kh : (c + 1) * kh, :n]
                turned[c, kh:] = b[c * kh : (c + 1) * kh, n:]
                g = dot(t_three[...], turned[c])
                pr, pi = probes[d, c, 0], probes[d, c, 1]
                placed[0] += pr * g[:n] + pi * g[n:]
                placed[1] += pr * g[n:] - pi * g[:n]
            return 0

        clear(placed)
        lax.fori_loop(0, n_ma, pair, 0)

    def place(it):
        def put(q, _):
            x = dot(put_rows[...], two_terms(placed[q], terms[2], 0))
            ext[it, q] = dot(two_terms(x, terms[3], 1), put_cols[...])
            return 0

        lax.fori_loop(0, 2, put, 0)

    quarter = tx // n_ma
    my_quarter = pl.ds(pl.multiple_of(rim + ma * quarter, quarter), quarter)

    def combine(it):
        place(it)
        sent = []
        for p in range(2):
            low = copies.make(
                ext.at[it, p, pl.ds(0, rim)], from_z.at[it, 0, p], {"gx": gx - 1}, up
            )
            high = copies.make(
                ext.at[it, p, pl.ds(rim + tx, rim)], from_z.at[it, 1, p], {"gx": gx + 1}, down
            )
            when(up, low.start)
            when(down, high.start)
            sent.append(((down, low), (up, high)))
        beside = []
        for p in range(2):
            arrive(sent[p])
            ext[it, p, own_rows] += from_z[it, 0, p] + from_z[it, 1, p]
            low = copies.make(
                ext.at[it, p, own_rows, pl.ds(0, rim)], from_y.at[it, 0, p], {"gy": gy - 1}, left
            )
            high = copies.make(
                ext.at[it, p, own_rows, pl.ds(rim + ty, rim)],
                from_y.at[it, 1, p],
                {"gy": gy + 1},
                right,
            )
            when(left, low.start)
            when(right, high.start)
            beside.append(((right, low), (left, high)))
        quarters = []
        for p in range(2):
            arrive(beside[p])
            ext[it, p, own_rows, pl.ds(ty, rim)] += from_y[it, 0, p]
            ext[it, p, own_rows, pl.ds(rim, rim)] += from_y[it, 1, p]
            batch = []
            for o in range(1, n_ma):
                peer = lax.rem(ma + o, n_ma)
                rows = pl.ds(pl.multiple_of(rim + peer * quarter, quarter), quarter)
                copy = copies.make(
                    ext.at[it, p, rows, own_cols], from_ma.at[it, o - 1, p], {"ma": peer}
                )
                copy.start()
                batch.append(copy)
            quarters.append(batch)
        gathers, square = [], jnp.zeros((8, 128), F32)
        for p in range(2):
            total = ext[it, p, my_quarter, own_cols]
            for o in range(1, n_ma):
                quarters[p][o - 1].wait_recv()
                total += from_ma[it, o - 1, p]
            dirs[it, p, my_quarter, own_cols] = -total
            square += squares(total)
            batch = []
            for o in range(1, n_ma):
                mine = dirs.at[it, p, my_quarter, own_cols]
                copy = copies.make(mine, mine, {"ma": lax.rem(ma + o, n_ma)})
                copy.start()
                batch.append(copy)
            gathers.append(batch)
        beside = []
        for p in range(2):
            for copy in gathers[p]:
                copy.wait_recv()
            beside.append(shift_y(dirs.at[it], p))
        widen_end(dirs.at[it], beside)
        return square

    def squares(x):
        x = x * x
        out = x[:, :128]
        for i in range(1, x.shape[1] // 128):
            out = out + x[:, i * 128 : (i + 1) * 128]
        return jnp.sum(out.reshape(-1, 8, 128), axis=0)

    def step_size(it, square, changes):
        value = jnp.stack([square, changes])
        for axis, size, me, buf in (
            ("ma", n_ma, ma, sums_ma),
            ("gy", n_gy, gy, sums_gy),
            ("gx", n_gx, gx, sums_gx),
        ):
            buf[it, me] = value
            batch = []
            for o in range(1, size):
                mine = buf.at[it, me]
                copy = copies.make(mine, mine, {axis: lax.rem(me + o, size)})
                copy.start()
                batch.append(copy)
            for copy in batch:
                copy.wait_recv()
            value = buf[it, 0]
            for i in range(1, size):
                value += buf[it, i]
        norm = jnp.sum(value[0], keepdims=True)
        return norm / (jnp.sum(value[1], keepdims=True) + DAMPING * norm)

    window(cur)
    intensity = jnp.zeros((kh, n), F32)

    def hand(d, part):
        copy = copies.make(probes.at[d, core, part], probes.at[d, core, part], partner)
        copy.start()
        return copy

    handed = {}
    for part, other in ((0, 1), (1, 0)):
        ring["n", part].wait_recv()
        ring["p", other].wait_recv()
        if part == 0:
            forth = copies.make(probes.at[1, core, 0], probes.at[2, core, 0], ma_next)
            back = copies.make(probes.at[3, core, 1], probes.at[2, core, 1], ma_prev)
            forth.start()
            back.start()
        handed[1, part] = hand(1, part)
        handed[3, other] = hand(3, other)
        if part == 0:
            f = forward_pair(0)
            spec[pair_rows(0), :] = f
            intensity += folded(f * f)
    for d in (1, 3):
        handed[d, 0].wait_recv()
        handed[d, 1].wait_recv()
        f = forward_pair(d)
        spec[pair_rows(d), :] = f
        intensity += folded(f * f)
    forth.wait_recv()
    handed[2, 0] = hand(2, 0)
    back.wait_recv()
    handed[2, 1] = hand(2, 1)
    handed[2, 0].wait_recv()
    handed[2, 1].wait_recv()
    f = forward_pair(2)
    spec[pair_rows(2), :] = f
    intensity += folded(f * f)

    for it in range(OUTER):
        backward(live * (intensity - meas[...]))
        square = combine(it)
        window(dirs.at[it])
        last = it + 1 == OUTER

        def pair(d, change, last=last):
            m = forward_pair(d)
            if not last:
                moved[pair_rows(d), :] = m
            return change + folded(spec[pair_rows(d), :] * m)

        change = live * 2.0 * lax.fori_loop(0, n_ma, pair, jnp.zeros((kh, n), F32))
        alpha = step_size(it, square, squares(change))
        obj[...] += alpha * dirs[it, :, own_rows, own_cols]
        if not last:

            def advance(d, total, alpha=alpha):
                f = spec[pair_rows(d), :] + alpha * moved[pair_rows(d), :]
                spec[pair_rows(d), :] = f
                return total + folded(f * f)

            intensity = lax.fori_loop(0, n_ma, advance, jnp.zeros((kh, n), F32))
    out_ref[...] = obj[...]
    copies.finish()


def solution(mesh):
    sizes = (mesh.shape["gx"], mesh.shape["gy"], mesh.shape["ma"])

    def shards(object_field, probe_modes, measured, positions, slot_counts):
        n = probe_modes.shape[-1]
        _, tx, ty = object_field.shape
        rim, kh = n // 2, n // 2
        wide = (2, tx + 2 * rim, ty + 2 * rim)
        modes = probe_modes.shape[0] * sizes[2]
        quarter = tx // sizes[2]
        vmem = pltpu.VMEM
        scratch = [
            vmem((2, tx, ty), F32),
            vmem(wide, F32),
            vmem((sizes[2], 2, 2, n, n), F32),
            vmem((kh, n), F32),
            vmem((n, 2 * n), BF16),
            vmem((2 * n, 2 * n), BF16),
            vmem((2 * n, 2 * n), BF16),
            vmem((2 * n, n), BF16),
            vmem((2, n, n), F32),
            vmem((2, 2 * n, n), BF16),
            vmem((n, 2 * n), BF16),
            vmem((modes * kh, 2 * n), F32),
            vmem((modes * kh, 2 * n), F32),
            vmem((2, n, n), BF16),
            vmem((kh, 2 * n), F32),
            vmem((2, n, n), F32),
            vmem((n, 2 * wide[1]), BF16),
            vmem((2 * wide[2], n), BF16),
            vmem((wide[1], 2 * n), BF16),
            vmem((2 * n, wide[2]), BF16),
            vmem((wide[1], 2 * wide[2]), BF16),
            vmem((2 * wide[1], n), BF16),
            vmem((2 * n, n), BF16),
            vmem((wide[1], 2 * n), BF16),
            vmem((OUTER, *wide), F32),
            vmem((OUTER, *wide), F32),
            vmem((OUTER, 2, 2, tx, ty + 2 * rim), F32),
            vmem((OUTER, 2, 2, tx, rim), F32),
            vmem((OUTER, sizes[2] - 1, 2, quarter, ty), F32),
            vmem((OUTER, sizes[2], 2, 8, 128), F32),
            vmem((OUTER, sizes[1], 2, 8, 128), F32),
            vmem((OUTER, sizes[0], 2, 8, 128), F32),
            pltpu.SemaphoreType.DMA((4,)),
            pltpu.SemaphoreType.DMA((128,)),
            pltpu.SemaphoreType.DMA((128,)),
        ]
        anywhere = pl.BlockSpec(memory_space=pl.ANY)
        smem = pl.BlockSpec(memory_space=pltpu.SMEM)
        in_vmem = pl.BlockSpec(memory_space=pltpu.VMEM)
        return pl.pallas_call(
            functools.partial(kernel, (*sizes, n, tx, ty)),
            out_shape=jax.ShapeDtypeStruct(object_field.shape, F32),
            in_specs=[anywhere, anywhere, anywhere, smem, smem, in_vmem],
            out_specs=in_vmem,
            scratch_shapes=scratch,
            compiler_params=pltpu.CompilerParams(
                collective_id=0, has_side_effects=True, vmem_limit_bytes=60 * 1024 * 1024
            ),
        )(object_field, probe_modes, measured, positions, slot_counts, jnp.asarray(dft_parts(n)))

    placed = (
        P(None, "gx", "gy"),
        P("ma", None, None, None),
        P("gx", "gy", None, None, None),
        P("gx", "gy", None, None),
        P("gx", "gy"),
    )
    return jax.shard_map(
        shards, mesh=mesh, in_specs=placed, out_specs=P(None, "gx", "gy"), check_vma=False
    )
```

```python
import functools
import math

import jax
import jax.numpy as jnp
import numpy as np
from jax import lax
from jax.experimental import pallas as pl
from jax.experimental.pallas import tpu as pltpu
from jax.sharding import PartitionSpec as P

OUTER = 2
DAMPING = 1.0
MESH = pl.DeviceIdType.MESH
F32 = jnp.float32
BF16 = jnp.bfloat16


def dft_parts(n):
    ladder = np.arange(n, dtype=np.int32)
    phases = ladder[:, None] * ladder[None, :] % n
    angles = phases.astype(np.float32) * np.float32(2.0 * math.pi / n)
    factor = np.float32(1.0 / math.sqrt(n))
    return np.stack([np.cos(angles) * factor, -np.sin(angles) * factor]).astype(BF16)


class Copies:
    def __init__(self, send_sems, recv_sems):
        self.send_sems, self.recv_sems, self.count, self.pending = send_sems, recv_sems, 0, []

    def make(self, src, dst, device, sends=None):
        copy = pltpu.make_async_remote_copy(
            src_ref=src,
            dst_ref=dst,
            send_sem=self.send_sems.at[self.count],
            recv_sem=self.recv_sems.at[self.count],
            device_id=device,
            device_id_type=MESH,
        )
        self.count += 1
        self.pending.append((copy, sends))
        return copy

    def finish(self):
        for copy, sends in self.pending:
            when(sends, copy.wait_send)
        self.pending = []


def when(condition, action):
    if condition is None:
        action()
    else:
        pl.when(condition)(action)


def kernel(
    dims,
    obj_hbm,
    probe_hbm,
    meas_hbm,
    pos_ref,
    count_ref,
    w_ref,
    out_ref,
    obj,
    wide,
    cut,
    lent,
    probes,
    meas,
    t_one,
    t_two,
    t_back,
    t_three,
    win,
    wave,
    half,
    spec,
    moved,
    turned,
    weight,
    patch,
    tall,
    cut_rows,
    cut_cols,
    put_rows,
    put_cols,
    columns,
    terms_cols,
    terms_rows,
    terms_patch,
    terms_put,
    ext,
    from_z,
    from_y,
    from_ma,
    sums_plane,
    sums_line,
    local_sems,
    send_sems,
    recv_sems,
):
    n_gx, n_gy, n_ma, n, tx, ty = dims
    rim = n // 2
    kh = n // 2
    gx, gy, ma = lax.axis_index("gx"), lax.axis_index("gy"), lax.axis_index("ma")
    core = lax.rem(gx, 2)
    slot, part_k = ma // 2, lax.rem(ma, 2)
    up, down = gx > 0, gx < n_gx - 1
    left, right = gy > 0, gy < n_gy - 1
    copies = Copies(send_sems, recv_sems)
    row_chunk = tx // 2
    chunks = [(p, j * row_chunk) for p in range(2) for j in range(2)]

    barrier = pltpu.get_barrier_semaphore()
    line = [{"gx": lax.rem(gx + o, n_gx)} for o in range(1, n_gx)]
    plane = [
        {"gy": lax.rem(gy + o // n_ma, n_gy), "ma": lax.rem(ma + o % n_ma, n_ma)}
        for o in range(1, n_gy * n_ma)
    ]
    for device in line + plane:
        pl.semaphore_signal(barrier, inc=1, device_id=device, device_id_type=MESH)

    k_rows = pl.ds(pl.multiple_of(part_k * kh, kh), kh)
    own_cols = pl.ds(rim, ty)
    loads = [
        pltpu.make_async_copy(obj_hbm, wide.at[0, :, :, own_cols], local_sems.at[0]),
        pltpu.make_async_copy(probe_hbm, probes.at[0], local_sems.at[1]),
        pltpu.make_async_copy(obj_hbm, obj, local_sems.at[2]),
        pltpu.make_async_copy(meas_hbm.at[0, 0, slot, k_rows], meas, local_sems.at[3]),
    ]
    for load in loads:
        load.start()
    row_at, col_at = pos_ref[0, 0, slot, 0], pos_ref[0, 0, slot, 1]
    live = jnp.where(slot < count_ref[0, 0], 1.0, 0.0).astype(F32)
    columns[0] = jnp.full((8, 128), col_at.astype(F32))
    for load in loads:
        load.wait()
    pl.semaphore_wait(barrier, len(line) + len(plane))

    ma_next, ma_prev = {"ma": lax.rem(ma + 1, n_ma)}, {"ma": lax.rem(ma + n_ma - 1, n_ma)}
    partner = {"gx": gx + 1 - 2 * core}
    ring = {}
    for part, other in ((0, 1), (1, 0)):
        ring["n", part] = copies.make(probes.at[0, core, part], probes.at[1, core, part], ma_next)
        ring["p", other] = copies.make(probes.at[0, core, other], probes.at[3, core, other], ma_prev)
        ring["n", part].start()
        ring["p", other].start()

    above = copies.make(columns.at[0], columns.at[2], {"gx": gx - 1}, up)
    below = copies.make(columns.at[0], columns.at[1], {"gx": gx + 1}, down)
    when(up, above.start)
    when(down, below.start)

    def exchange(condition_low, condition_high, axis, me, low, high):
        first = copies.make(*low, {axis: me - 1}, condition_low)
        second = copies.make(*high, {axis: me + 1}, condition_high)
        when(condition_low, first.start)
        when(condition_high, second.start)
        return ((condition_high, first), (condition_low, second))

    def arrive(arrivals):
        for condition, copy in arrivals:
            when(condition, copy.wait_recv)

    def beside(buf, p, at, rows):
        strip = buf.at[p, pl.ds(at, rows)]
        return exchange(
            left,
            right,
            "gy",
            gy,
            (strip.at[:, pl.ds(rim, rim)], strip.at[:, pl.ds(rim + ty, rim)]),
            (strip.at[:, pl.ds(ty, rim)], strip.at[:, pl.ds(0, rim)]),
        )

    first_beside = [beside(wide.at[0], p, 0, tx) for p in range(2)]

    w_re, w_im = w_ref[0], w_ref[1]
    t_two[:n, :n], t_two[:n, n:], t_two[n:, :n], t_two[n:, n:] = w_re, w_im, -w_im, w_re
    t_back[:n, :n], t_back[:n, n:], t_back[n:, :n], t_back[n:, n:] = w_re, -w_im, w_im, w_re
    wk_re, wk_im = w_ref[0, k_rows, :], w_ref[1, k_rows, :]
    t_one[:kh, :n], t_one[:kh, n:], t_one[kh:, :n], t_one[kh:, n:] = wk_re, -wk_im, wk_im, wk_re
    k_cols = pl.ds(pl.multiple_of(part_k * kh, kh), kh)
    wc_re, wc_im = w_ref[0, :, k_cols], w_ref[1, :, k_cols]
    t_three[:n, :kh], t_three[:n, kh:] = wc_re, wc_im
    t_three[n:, :kh], t_three[n:, kh:] = -wc_im, wc_re

    def clear(ref):
        ref[...] = jnp.zeros(ref.shape, ref.dtype)

    for it in range(OUTER + 1):
        for p in range(2):
            when(gx == 0, functools.partial(clear, cut.at[it, p, pl.ds(0, rim)]))
            when(gx == n_gx - 1, functools.partial(clear, cut.at[it, p, pl.ds(rim + tx, rim)]))
            when(gy == 0, functools.partial(clear, wide.at[it, p, :, pl.ds(0, rim)]))
            when(gy == n_gy - 1, functools.partial(clear, wide.at[it, p, :, pl.ds(rim + ty, rim)]))
            if it < OUTER:
                when(gx == n_gx - 1, functools.partial(clear, from_z.at[it, 0, p]))
                when(gx == 0, functools.partial(clear, from_z.at[it, 1, p]))
                when(gy == n_gy - 1, functools.partial(clear, from_y.at[it, 0, p]))
                when(gy == 0, functools.partial(clear, from_y.at[it, 1, p]))
    when(gx == 0, functools.partial(clear, columns.at[1]))
    when(gx == n_gx - 1, functools.partial(clear, columns.at[2]))

    height, width = 2 * rim + tx, 2 * rim + ty

    def chosen(shape, dim, first):
        here = lax.broadcasted_iota(jnp.int32, shape, dim)
        there = lax.broadcasted_iota(jnp.int32, shape, 1 - dim)
        return jnp.where((here - there).astype(F32) == first, 1.0, 0.0).astype(BF16)

    row_first = jnp.full((1, 1), row_at.astype(F32))
    for i in range(2):
        cut_rows[:, i * height : (i + 1) * height] = chosen((n, height), 1, row_first)
        put_rows[:, i * n : (i + 1) * n] = chosen((height, n), 0, row_first)
    arrive(((down, above), (up, below)))
    for which in range(3):
        first = columns[which][:1, :1]
        for i in range(2):
            cut_cols[i * width : (i + 1) * width, which * n : (which + 1) * n] = chosen(
                (width, n), 0, first
            )
            at = (2 * which + i) * n
            put_cols[at : at + n] = chosen((n, width), 1, first)

    def two_terms(x, ref, at, axis):
        top = x.astype(BF16)
        rest = (x - top.astype(F32)).astype(BF16)
        size = x.shape[axis]
        if axis == 0:
            ref[at : at + size], ref[at + size : at + 2 * size] = top, rest
        else:
            ref[:, at : at + size], ref[:, at + size : at + 2 * size] = top, rest

    def dot(x, y):
        return jnp.dot(x, y, preferred_element_type=F32)

    def cut_and_lend(it, p, at):
        rows = pl.ds(at, row_chunk)
        two_terms(wide[it, p, rows], terms_cols, 0, 1)
        x = dot(terms_cols[...], cut_cols[...])
        cut[it, p, pl.ds(rim + at, row_chunk)] = x[:, :n]
        lent[it, 0, p, rows] = x[:, n : 2 * n]
        lent[it, 1, p, rows] = x[:, 2 * n :]
        return exchange(
            up,
            down,
            "gx",
            gx,
            (lent.at[it, 0, p, rows], cut.at[it, p, pl.ds(rim + tx + at, row_chunk)]),
            (lent.at[it, 1, p, rows], cut.at[it, p, pl.ds(at, row_chunk)]),
        )

    def window(it):
        def part(p, _):
            two_terms(cut[it, p], terms_rows, 0, 0)
            win[p] = dot(cut_rows[...], terms_rows[...])
            return 0

        lax.fori_loop(0, 2, part, 0)

    for p in range(2):
        arrive(first_beside[p])
    stacked = [cut_and_lend(0, p, at) for p, at in chunks]
    for arrivals in stacked:
        arrive(arrivals)

    def forward_pair(d):
        for c in range(2):
            pr, pi = probes[d, c, 0], probes[d, c, 1]
            wr, wi = win[0], win[1]
            wave[c, :n] = (pr * wr - pi * wi).astype(BF16)
            wave[c, n:] = (pr * wi + pi * wr).astype(BF16)
            h = dot(t_one[...], wave[c]).astype(BF16)
            half[c * kh : (c + 1) * kh, :n] = h[:kh]
            half[c * kh : (c + 1) * kh, n:] = h[kh:]
        return dot(half[...], t_two[...])

    def pair_rows(d):
        return pl.ds(pl.multiple_of(d * n, n), n)

    def folded(x):
        x = x[:kh] + x[kh:]
        return x[:, :n] + x[:, n:]

    def backward(misfit):
        weight[:, :n] = 2.0 * misfit
        weight[:, n:] = 2.0 * misfit

        def pair(d, _):
            y = weight[...]
            f = spec[pair_rows(d), :]
            half[:kh] = (f[:kh] * y).astype(BF16)
            half[kh:] = (f[kh:] * y).astype(BF16)
            b = dot(half[...], t_back[...]).astype(BF16)
            for c in range(2):
                turned[c, :kh] = b[c * kh : (c + 1) * kh, :n]
                turned[c, kh:] = b[c * kh : (c + 1) * kh, n:]
                g = dot(t_three[...], turned[c])
                pr, pi = probes[d, c, 0], probes[d, c, 1]
                patch[0] += pr * g[:n] + pi * g[n:]
                patch[1] += pr * g[n:] - pi * g[:n]
            return 0

        clear(patch)
        lax.fori_loop(0, n_ma, pair, 0)

    def place(it):
        def part(p, _):
            two_terms(patch[p], terms_patch, 0, 0)
            tall[it, p] = dot(put_rows[...], terms_patch[...])
            return 0

        lax.fori_loop(0, 2, part, 0)

    def combine(it):
        place(it)
        folds = []
        for p, at in chunks:
            rows = pl.ds(at, row_chunk)
            folds.append(
                exchange(
                    up,
                    down,
                    "gx",
                    gx,
                    (tall.at[it, p, rows], from_z.at[it, 0, p, rows]),
                    (tall.at[it, p, pl.ds(rim + tx + at, row_chunk)], from_z.at[it, 1, p, rows]),
                )
            )
        sides = []
        for i, (p, at) in enumerate(chunks):
            rows = pl.ds(at, row_chunk)
            arrive(folds[i])
            two_terms(tall[it, p, pl.ds(rim + at, row_chunk)], terms_put, 0, 1)
            two_terms(from_z[it, 1, p, rows], terms_put, 2 * n, 1)
            two_terms(from_z[it, 0, p, rows], terms_put, 4 * n, 1)
            ext[it, p, rows] = dot(terms_put[...], put_cols[...])
            strip = ext.at[it, p, rows]
            sides.append(
                exchange(
                    left,
                    right,
                    "gy",
                    gy,
                    (strip.at[:, pl.ds(0, rim)], from_y.at[it, 0, p, rows]),
                    (strip.at[:, pl.ds(rim + ty, rim)], from_y.at[it, 1, p, rows]),
                )
            )
        share = row_chunk // n_ma
        parts = []
        for i, (p, at) in enumerate(chunks):
            rows = pl.ds(at, row_chunk)
            arrive(sides[i])
            ext[it, p, rows, pl.ds(ty, rim)] += from_y[it, 0, p, rows]
            ext[it, p, rows, pl.ds(rim, rim)] += from_y[it, 1, p, rows]
            batch = []
            for o in range(1, n_ma):
                peer = lax.rem(ma + o, n_ma)
                theirs = pl.ds(pl.multiple_of(at + peer * share, share), share)
                copy = copies.make(
                    ext.at[it, p, theirs, own_cols], from_ma.at[it, o - 1, i], {"ma": peer}
                )
                copy.start()
                batch.append(copy)
            parts.append(batch)
        gathers, square = [], jnp.zeros((8, 128), F32)
        for i, (p, at) in enumerate(chunks):
            mine = pl.ds(pl.multiple_of(at + ma * share, share), share)
            total = ext[it, p, mine, own_cols]
            for o in range(1, n_ma):
                parts[i][o - 1].wait_recv()
                total += from_ma[it, o - 1, i]
            wide[it + 1, p, mine, own_cols] = -total
            square += squares(total)
            batch = []
            for o in range(1, n_ma):
                ours = wide.at[it + 1, p, mine, own_cols]
                copy = copies.make(ours, ours, {"ma": lax.rem(ma + o, n_ma)})
                copy.start()
                batch.append(copy)
            gathers.append(batch)
        sides = []
        for i, (p, at) in enumerate(chunks):
            for copy in gathers[i]:
                copy.wait_recv()
            sides.append(beside(wide.at[it + 1], p, at, row_chunk))
        stacked = []
        for i, (p, at) in enumerate(chunks):
            arrive(sides[i])
            stacked.append(cut_and_lend(it + 1, p, at))
        for arrivals in stacked:
            arrive(arrivals)
        return square

    def squares(x):
        x = x * x
        out = x[:, :128]
        for i in range(1, x.shape[1] // 128):
            out = out + x[:, i * 128 : (i + 1) * 128]
        return jnp.sum(out.reshape(-1, 8, 128), axis=0)

    def row_of(x):
        x = jnp.sum(x, axis=0, keepdims=True)
        return x + pltpu.roll(x, 64, 1)

    def step_size(it, square, changes):
        lane = lax.broadcasted_iota(jnp.int32, (1, 128), 1)
        value = jnp.where(lane < 64, row_of(square), row_of(changes))
        for buf, me, devices in (
            (sums_plane, gy * n_ma + ma, plane),
            (sums_line, gx, line),
        ):
            buf[it, me] = value
            batch = []
            for device in devices:
                mine = buf.at[it, me]
                copy = copies.make(mine, mine, device)
                copy.start()
                batch.append(copy)
            for copy in batch:
                copy.wait_recv()
            value = buf[it, 0]
            for i in range(1, len(devices) + 1):
                value += buf[it, i]
        norm = jnp.sum(jnp.where(lane < 64, value, 0.0), keepdims=True)
        change = jnp.sum(jnp.where(lane < 64, 0.0, value), keepdims=True)
        return norm / (change + DAMPING * norm)

    window(0)
    intensity = jnp.zeros((kh, n), F32)

    def hand(d, part):
        copy = copies.make(probes.at[d, core, part], probes.at[d, core, part], partner)
        copy.start()
        return copy

    handed = {}
    for part, other in ((0, 1), (1, 0)):
        ring["n", part].wait_recv()
        ring["p", other].wait_recv()
        if part == 0:
            forth = copies.make(probes.at[1, core, 0], probes.at[2, core, 0], ma_next)
            back = copies.make(probes.at[3, core, 1], probes.at[2, core, 1], ma_prev)
            forth.start()
            back.start()
        handed[1, part] = hand(1, part)
        handed[3, other] = hand(3, other)
        if part == 0:
            f = forward_pair(0)
            spec[pair_rows(0), :] = f
            intensity += folded(f * f)
    for d in (1, 3):
        handed[d, 0].wait_recv()
        handed[d, 1].wait_recv()
        f = forward_pair(d)
        spec[pair_rows(d), :] = f
        intensity += folded(f * f)
    forth.wait_recv()
    handed[2, 0] = hand(2, 0)
    back.wait_recv()
    handed[2, 1] = hand(2, 1)
    handed[2, 0].wait_recv()
    handed[2, 1].wait_recv()
    f = forward_pair(2)
    spec[pair_rows(2), :] = f
    intensity += folded(f * f)

    for it in range(OUTER):
        backward(live * (intensity - meas[...]))
        square = combine(it)
        window(it + 1)
        last = it + 1 == OUTER

        def pair(d, change, last=last):
            m = forward_pair(d)
            if not last:
                moved[pair_rows(d), :] = m
            return change + folded(spec[pair_rows(d), :] * m)

        change = live * 2.0 * lax.fori_loop(0, n_ma, pair, jnp.zeros((kh, n), F32))
        alpha = step_size(it, square, squares(change))
        obj[...] += alpha * wide[it + 1, :, :, own_cols]
        if not last:

            def advance(d, total, alpha=alpha):
                f = spec[pair_rows(d), :] + alpha * moved[pair_rows(d), :]
                spec[pair_rows(d), :] = f
                return total + folded(f * f)

            intensity = lax.fori_loop(0, n_ma, advance, jnp.zeros((kh, n), F32))
    out_ref[...] = obj[...]
    copies.finish()


def solution(mesh):
    sizes = (mesh.shape["gx"], mesh.shape["gy"], mesh.shape["ma"])

    def shards(object_field, probe_modes, measured, positions, slot_counts):
        n = probe_modes.shape[-1]
        _, tx, ty = object_field.shape
        rim, kh = n // 2, n // 2
        height, width = tx + 2 * rim, ty + 2 * rim
        modes = probe_modes.shape[0] * sizes[2]
        row_chunk = tx // 2
        vmem = pltpu.VMEM
        scratch = [
            vmem((2, tx, ty), F32),
            vmem((OUTER + 1, 2, tx, width), F32),
            vmem((OUTER + 1, 2, height, n), F32),
            vmem((OUTER + 1, 2, 2, tx, n), F32),
            vmem((sizes[2], 2, 2, n, n), F32),
            vmem((kh, n), F32),
            vmem((n, 2 * n), BF16),
            vmem((2 * n, 2 * n), BF16),
            vmem((2 * n, 2 * n), BF16),
            vmem((2 * n, n), BF16),
            vmem((2, n, n), F32),
            vmem((2, 2 * n, n), BF16),
            vmem((n, 2 * n), BF16),
            vmem((modes * kh, 2 * n), F32),
            vmem((modes * kh, 2 * n), F32),
            vmem((2, n, n), BF16),
            vmem((kh, 2 * n), F32),
            vmem((2, n, n), F32),
            vmem((OUTER, 2, height, n), F32),
            vmem((n, 2 * height), BF16),
            vmem((2 * width, 3 * n), BF16),
            vmem((height, 2 * n), BF16),
            vmem((6 * n, width), BF16),
            vmem((3, 8, 128), F32),
            vmem((row_chunk, 2 * width), BF16),
            vmem((2 * height, n), BF16),
            vmem((2 * n, n), BF16),
            vmem((row_chunk, 6 * n), BF16),
            vmem((OUTER, 2, tx, width), F32),
            vmem((OUTER, 2, 2, tx, n), F32),
            vmem((OUTER, 2, 2, tx, rim), F32),
            vmem((OUTER, sizes[2] - 1, 4, row_chunk // sizes[2], ty), F32),
            vmem((OUTER, sizes[1] * sizes[2], 1, 128), F32),
            vmem((OUTER, sizes[0], 1, 128), F32),
            pltpu.SemaphoreType.DMA((4,)),
            pltpu.SemaphoreType.DMA((208,)),
            pltpu.SemaphoreType.DMA((208,)),
        ]
        anywhere = pl.BlockSpec(memory_space=pl.ANY)
        smem = pl.BlockSpec(memory_space=pltpu.SMEM)
        in_vmem = pl.BlockSpec(memory_space=pltpu.VMEM)
        return pl.pallas_call(
            functools.partial(kernel, (*sizes, n, tx, ty)),
            out_shape=jax.ShapeDtypeStruct(object_field.shape, F32),
            in_specs=[anywhere, anywhere, anywhere, smem, smem, in_vmem],
            out_specs=in_vmem,
            scratch_shapes=scratch,
            compiler_params=pltpu.CompilerParams(
                collective_id=0, has_side_effects=True, vmem_limit_bytes=60 * 1024 * 1024
            ),
        )(object_field, probe_modes, measured, positions, slot_counts, jnp.asarray(dft_parts(n)))

    placed = (
        P(None, "gx", "gy"),
        P("ma", None, None, None),
        P("gx", "gy", None, None, None),
        P("gx", "gy", None, None),
        P("gx", "gy"),
    )
    return jax.shard_map(
        shards, mesh=mesh, in_specs=placed, out_specs=P(None, "gx", "gy"), check_vma=False
    )
```

```python
import functools
import math

import jax
import jax.numpy as jnp
import numpy as np
from jax import lax
from jax.experimental import pallas as pl
from jax.experimental.pallas import tpu as pltpu
from jax.sharding import PartitionSpec as P

OUTER = 2
DAMPING = 1.0
MESH = pl.DeviceIdType.MESH
F32 = jnp.float32
BF16 = jnp.bfloat16


def dft_parts(n):
    ladder = np.arange(n, dtype=np.int32)
    phases = ladder[:, None] * ladder[None, :] % n
    angles = phases.astype(np.float32) * np.float32(2.0 * math.pi / n)
    factor = np.float32(1.0 / math.sqrt(n))
    return np.stack([np.cos(angles) * factor, -np.sin(angles) * factor]).astype(BF16)


class Copies:
    def __init__(self, send_sems, recv_sems):
        self.send_sems, self.recv_sems, self.count, self.pending = send_sems, recv_sems, 0, []

    def make(self, src, dst, device, sends=None):
        copy = pltpu.make_async_remote_copy(
            src_ref=src,
            dst_ref=dst,
            send_sem=self.send_sems.at[self.count],
            recv_sem=self.recv_sems.at[self.count],
            device_id=device,
            device_id_type=MESH,
        )
        self.count += 1
        self.pending.append((copy, sends))
        return copy

    def finish(self):
        for copy, sends in self.pending:
            when(sends, copy.wait_send)
        self.pending = []


def when(condition, action):
    if condition is None:
        action()
    else:
        pl.when(condition)(action)


def kernel(
    dims,
    obj_hbm,
    probe_hbm,
    meas_hbm,
    pos_ref,
    count_ref,
    w_ref,
    out_ref,
    obj,
    wide,
    cut,
    lent,
    probes,
    meas,
    t_one,
    t_two,
    t_back,
    t_three,
    win,
    wave,
    half,
    spec,
    moved,
    turned,
    weight,
    patch,
    tall,
    cut_rows,
    cut_cols,
    put_rows,
    put_cols,
    columns,
    terms_cols,
    terms_rows,
    terms_patch,
    terms_put,
    ext,
    from_z,
    from_y,
    from_ma,
    sums_plane,
    sums_line,
    token,
    local_sems,
    send_sems,
    recv_sems,
):
    n_gx, n_gy, n_ma, n, tx, ty = dims
    rim = n // 2
    kh = n // 2
    gx, gy, ma = lax.axis_index("gx"), lax.axis_index("gy"), lax.axis_index("ma")
    core = lax.rem(gx, 2)
    slot, part_k = ma // 2, lax.rem(ma, 2)
    up, down = gx > 0, gx < n_gx - 1
    left, right = gy > 0, gy < n_gy - 1
    copies = Copies(send_sems, recv_sems)
    row_chunk = tx // 2
    chunks = [(p, j * row_chunk) for p in range(2) for j in range(2)]

    barrier = pltpu.get_barrier_semaphore()
    line = [{"gx": lax.rem(gx + o, n_gx)} for o in range(1, n_gx)]
    plane = [
        {"gy": lax.rem(gy + o // n_ma, n_gy), "ma": lax.rem(ma + o % n_ma, n_ma)}
        for o in range(1, n_gy * n_ma)
    ]

    def at_distance(axis, o):
        me, size = {"gx": (gx, n_gx), "gy": (gy, n_gy), "ma": (ma, n_ma)}[axis]
        offsets = {o % size, (size - o) % size}
        return [{axis: lax.rem(me + off, size)} for off in sorted(offsets)]

    def tell(sem, devices):
        for device in devices:
            pl.semaphore_signal(sem, inc=1, device_id=device, device_id_type=MESH)

    nearest = at_distance("gx", 1) + at_distance("gy", 1) + at_distance("ma", 1)
    tell(barrier, nearest)

    k_rows = pl.ds(pl.multiple_of(part_k * kh, kh), kh)
    own_cols = pl.ds(rim, ty)
    loads = [
        pltpu.make_async_copy(obj_hbm, wide.at[0, :, :, own_cols], local_sems.at[0]),
        pltpu.make_async_copy(probe_hbm, probes.at[0], local_sems.at[1]),
        pltpu.make_async_copy(obj_hbm, obj, local_sems.at[2]),
        pltpu.make_async_copy(meas_hbm.at[0, 0, slot, k_rows], meas, local_sems.at[3]),
    ]
    for load in loads:
        load.start()
    row_at, col_at = pos_ref[0, 0, slot, 0], pos_ref[0, 0, slot, 1]
    live = jnp.where(slot < count_ref[0, 0], 1.0, 0.0).astype(F32)
    columns[0] = jnp.full((8, 128), col_at.astype(F32))
    w_re, w_im = w_ref[0], w_ref[1]
    t_two[:n, :n], t_two[:n, n:], t_two[n:, :n], t_two[n:, n:] = w_re, w_im, -w_im, w_re
    t_back[:n, :n], t_back[:n, n:], t_back[n:, :n], t_back[n:, n:] = w_re, -w_im, w_im, w_re
    wk_re, wk_im = w_ref[0, k_rows, :], w_ref[1, k_rows, :]
    t_one[:kh, :n], t_one[:kh, n:], t_one[kh:, :n], t_one[kh:, n:] = wk_re, -wk_im, wk_im, wk_re
    k_cols = pl.ds(pl.multiple_of(part_k * kh, kh), kh)
    wc_re, wc_im = w_ref[0, :, k_cols], w_ref[1, :, k_cols]
    t_three[:n, :kh], t_three[:n, kh:] = wc_re, wc_im
    t_three[n:, :kh], t_three[n:, kh:] = -wc_im, wc_re

    def clear(ref):
        ref[...] = jnp.zeros(ref.shape, ref.dtype)

    for it in range(OUTER + 1):
        for p in range(2):
            when(gx == 0, functools.partial(clear, cut.at[it, p, pl.ds(0, rim)]))
            when(gx == n_gx - 1, functools.partial(clear, cut.at[it, p, pl.ds(rim + tx, rim)]))
            when(gy == 0, functools.partial(clear, wide.at[it, p, :, pl.ds(0, rim)]))
            when(gy == n_gy - 1, functools.partial(clear, wide.at[it, p, :, pl.ds(rim + ty, rim)]))
            if it < OUTER:
                when(gx == n_gx - 1, functools.partial(clear, from_z.at[it, 0, p]))
                when(gx == 0, functools.partial(clear, from_z.at[it, 1, p]))
                when(gy == n_gy - 1, functools.partial(clear, from_y.at[it, 0, p]))
                when(gy == 0, functools.partial(clear, from_y.at[it, 1, p]))
    when(gx == 0, functools.partial(clear, columns.at[1]))
    when(gx == n_gx - 1, functools.partial(clear, columns.at[2]))

    height, width = 2 * rim + tx, 2 * rim + ty

    def chosen(shape, dim, first):
        here = lax.broadcasted_iota(jnp.int32, shape, dim)
        there = lax.broadcasted_iota(jnp.int32, shape, 1 - dim)
        return jnp.where((here - there).astype(F32) == first, 1.0, 0.0).astype(BF16)

    row_first = jnp.full((1, 1), row_at.astype(F32))
    for i in range(2):
        cut_rows[:, i * height : (i + 1) * height] = chosen((n, height), 1, row_first)
        put_rows[:, i * n : (i + 1) * n] = chosen((height, n), 0, row_first)

    def set_columns(which):
        first = columns[which][:1, :1]
        cut_cols[:, which * n : (which + 1) * n] = chosen((width, n), 0, first)
        put_cols[which * n : (which + 1) * n] = chosen((n, width), 1, first)

    set_columns(0)

    for load in loads:
        load.wait()
    pl.semaphore_wait(barrier, len(nearest))

    ma_next, ma_prev = {"ma": lax.rem(ma + 1, n_ma)}, {"ma": lax.rem(ma + n_ma - 1, n_ma)}
    gy_next, gy_prev = {"gy": lax.rem(gy + 1, n_gy)}, {"gy": lax.rem(gy + n_gy - 1, n_gy)}
    partner = {"gx": gx + 1 - 2 * core}
    mine_part = lax.rem(gy, 2)
    halves = (pl.ds(0, kh), pl.ds(kh, kh))

    def piece(d, part, h):
        return probes.at[d, core, part, halves[h]]

    def send(src, dst, device):
        copy = copies.make(src, dst, device)
        copy.start()
        return copy

    ring = {}
    for h, g in ((0, 1), (1, 0)):
        ring[1, h] = send(piece(0, mine_part, h), piece(1, mine_part, h), ma_next)
        ring[3, g] = send(piece(0, mine_part, g), piece(3, mine_part, g), ma_prev)

    above = copies.make(columns.at[0], columns.at[2], {"gx": gx - 1}, up)
    below = copies.make(columns.at[0], columns.at[1], {"gx": gx + 1}, down)
    when(up, above.start)
    when(down, below.start)

    def exchange(condition_low, condition_high, axis, me, low, high):
        first = copies.make(*low, {axis: me - 1}, condition_low)
        second = copies.make(*high, {axis: me + 1}, condition_high)
        when(condition_low, first.start)
        when(condition_high, second.start)
        return ((condition_high, first), (condition_low, second))

    def arrive(arrivals):
        for condition, copy in arrivals:
            when(condition, copy.wait_recv)

    def beside(buf, p, at, rows):
        strip = buf.at[p, pl.ds(at, rows)]
        return exchange(
            left,
            right,
            "gy",
            gy,
            (strip.at[:, pl.ds(rim, rim)], strip.at[:, pl.ds(rim + ty, rim)]),
            (strip.at[:, pl.ds(ty, rim)], strip.at[:, pl.ds(0, rim)]),
        )

    first_beside = [beside(wide.at[0], p, 0, tx) for p in range(2)]

    tell(token.at[0], at_distance("gx", 1))
    tell(token.at[3], at_distance("gy", 1) + at_distance("ma", 1))
    pl.semaphore_wait(token.at[0], 2)
    tell(token.at[1], at_distance("gx", 2))
    pl.semaphore_wait(token.at[3], 4)
    tell(token.at[4], at_distance("gy", 2) + at_distance("ma", 2))
    pl.semaphore_wait(token.at[1], 2)
    tell(token.at[2], at_distance("gx", 4))
    pl.semaphore_wait(token.at[4], 2)
    pl.semaphore_wait(token.at[2], 2)


    def two_terms(x, ref, at, axis):
        top = x.astype(BF16)
        rest = (x - top.astype(F32)).astype(BF16)
        size = x.shape[axis]
        if axis == 0:
            ref[at : at + size], ref[at + size : at + 2 * size] = top, rest
        else:
            ref[:, at : at + size], ref[:, at + size : at + 2 * size] = top, rest

    def dot(x, y):
        return jnp.dot(x, y, preferred_element_type=F32)

    def stack(x, ref, at):
        rows, cols = x.shape
        top = x.astype(BF16)
        ref[:rows, at : at + cols] = top
        ref[rows:, at : at + cols] = (x - top.astype(F32)).astype(BF16)

    def both(x):
        rows = x.shape[0] // 2
        return x[:rows] + x[rows:]

    def cut_and_lend(it, p, at):
        rows = pl.ds(at, row_chunk)
        stack(wide[it, p, rows], terms_cols, 0)
        x = both(dot(terms_cols[...], cut_cols[...]))
        cut[it, p, pl.ds(rim + at, row_chunk)] = x[:, :n]
        lent[it, 0, p, rows] = x[:, n : 2 * n]
        lent[it, 1, p, rows] = x[:, 2 * n :]
        return exchange(
            up,
            down,
            "gx",
            gx,
            (lent.at[it, 0, p, rows], cut.at[it, p, pl.ds(rim + tx + at, row_chunk)]),
            (lent.at[it, 1, p, rows], cut.at[it, p, pl.ds(at, row_chunk)]),
        )

    def window(it):
        def part(p, _):
            two_terms(cut[it, p], terms_rows, 0, 0)
            win[p] = dot(cut_rows[...], terms_rows[...])
            return 0

        lax.fori_loop(0, 2, part, 0)

    def forward_pair(d):
        for c in range(2):
            pr, pi = probes[d, c, 0], probes[d, c, 1]
            wr, wi = win[0], win[1]
            wave[c, :n] = (pr * wr - pi * wi).astype(BF16)
            wave[c, n:] = (pr * wi + pi * wr).astype(BF16)
            h = dot(t_one[...], wave[c]).astype(BF16)
            half[c * kh : (c + 1) * kh, :n] = h[:kh]
            half[c * kh : (c + 1) * kh, n:] = h[kh:]
        return dot(half[...], t_two[...])

    def pair_rows(d):
        return pl.ds(pl.multiple_of(d * n, n), n)

    def folded(x):
        x = x[:kh] + x[kh:]
        return x[:, :n] + x[:, n:]

    def backward(misfit, alpha):
        weight[:, :n] = 2.0 * misfit
        weight[:, n:] = 2.0 * misfit

        def pair(d, _):
            y = weight[...]
            f = spec[pair_rows(d), :]
            if alpha is not None:
                f = f + alpha * moved[pair_rows(d), :]
                spec[pair_rows(d), :] = f
            half[:kh] = (f[:kh] * y).astype(BF16)
            half[kh:] = (f[kh:] * y).astype(BF16)
            b = dot(half[...], t_back[...]).astype(BF16)
            for c in range(2):
                turned[c, :kh] = b[c * kh : (c + 1) * kh, :n]
                turned[c, kh:] = b[c * kh : (c + 1) * kh, n:]
                g = dot(t_three[...], turned[c])
                pr, pi = probes[d, c, 0], probes[d, c, 1]
                patch[0] += pr * g[:n] + pi * g[n:]
                patch[1] += pr * g[n:] - pi * g[:n]
            return 0

        clear(patch)
        lax.fori_loop(0, n_ma, pair, 0, unroll=True)

    def place(it):
        def part(p, _):
            two_terms(patch[p], terms_patch, 0, 0)
            tall[it, p] = dot(put_rows[...], terms_patch[...])
            return 0

        lax.fori_loop(0, 2, part, 0)

    def combine(it):
        place(it)
        folds = []
        for p, at in chunks:
            rows = pl.ds(at, row_chunk)
            folds.append(
                exchange(
                    up,
                    down,
                    "gx",
                    gx,
                    (tall.at[it, p, rows], from_z.at[it, 0, p, rows]),
                    (tall.at[it, p, pl.ds(rim + tx + at, row_chunk)], from_z.at[it, 1, p, rows]),
                )
            )
        sides = []
        for i, (p, at) in enumerate(chunks):
            rows = pl.ds(at, row_chunk)
            arrive(folds[i])
            stack(tall[it, p, pl.ds(rim + at, row_chunk)], terms_put, 0)
            stack(from_z[it, 1, p, rows], terms_put, n)
            stack(from_z[it, 0, p, rows], terms_put, 2 * n)
            ext[it, p, rows] = both(dot(terms_put[...], put_cols[...]))
            strip = ext.at[it, p, rows]
            sides.append(
                exchange(
                    left,
                    right,
                    "gy",
                    gy,
                    (strip.at[:, pl.ds(0, rim)], from_y.at[it, 0, p, rows]),
                    (strip.at[:, pl.ds(rim + ty, rim)], from_y.at[it, 1, p, rows]),
                )
            )
        share = row_chunk // n_ma
        parts = []
        for i, (p, at) in enumerate(chunks):
            rows = pl.ds(at, row_chunk)
            arrive(sides[i])
            ext[it, p, rows, pl.ds(ty, rim)] += from_y[it, 0, p, rows]
            ext[it, p, rows, pl.ds(rim, rim)] += from_y[it, 1, p, rows]
            batch = []
            for o in range(1, n_ma):
                peer = lax.rem(ma + o, n_ma)
                theirs = pl.ds(pl.multiple_of(at + peer * share, share), share)
                copy = copies.make(
                    ext.at[it, p, theirs, own_cols], from_ma.at[it, o - 1, i], {"ma": peer}
                )
                copy.start()
                batch.append(copy)
            parts.append(batch)
        gathers, square = [], jnp.zeros((8, 128), F32)
        for i, (p, at) in enumerate(chunks):
            mine = pl.ds(pl.multiple_of(at + ma * share, share), share)
            total = ext[it, p, mine, own_cols]
            for o in range(1, n_ma):
                parts[i][o - 1].wait_recv()
                total += from_ma[it, o - 1, i]
            wide[it + 1, p, mine, own_cols] = -total
            square += squares(total)
            batch = []
            for o in range(1, n_ma):
                ours = wide.at[it + 1, p, mine, own_cols]
                copy = copies.make(ours, ours, {"ma": lax.rem(ma + o, n_ma)})
                copy.start()
                batch.append(copy)
            gathers.append(batch)
        sides = []
        for i, (p, at) in enumerate(chunks):
            for copy in gathers[i]:
                copy.wait_recv()
            sides.append(beside(wide.at[it + 1], p, at, row_chunk))
        stacked = []
        for i, (p, at) in enumerate(chunks):
            arrive(sides[i])
            stacked.append(cut_and_lend(it + 1, p, at))
        for arrivals in stacked:
            arrive(arrivals)
        return square

    def squares(x):
        x = x * x
        out = x[:, :128]
        for i in range(1, x.shape[1] // 128):
            out = out + x[:, i * 128 : (i + 1) * 128]
        return jnp.sum(out.reshape(-1, 8, 128), axis=0)

    def row_of(x):
        x = jnp.sum(x, axis=0, keepdims=True)
        return x + pltpu.roll(x, 64, 1)

    def step_size(it, square, changes):
        lane = lax.broadcasted_iota(jnp.int32, (1, 128), 1)
        value = jnp.where(lane < 64, row_of(square), row_of(changes))
        for buf, me, devices in (
            (sums_plane, gy * n_ma + ma, plane),
            (sums_line, gx, line),
        ):
            buf[it, me] = value
            mine = buf.at[it, me]
            batch = [send(mine, mine, device) for device in devices]
            if devices is plane:
                yield
            for copy in batch:
                copy.wait_recv()
            value = buf[it, 0]
            for i in range(1, len(devices) + 1):
                value += buf[it, i]
        norm = jnp.sum(jnp.where(lane < 64, value, 0.0), keepdims=True)
        change = jnp.sum(jnp.where(lane < 64, 0.0, value), keepdims=True)
        yield norm / (change + DAMPING * norm)

    intensity = jnp.zeros((kh, n), F32)

    def add_spectra(d, total):
        f = forward_pair(d)
        spec[pair_rows(d), :] = f
        return total + folded(f * f)

    other_part = 1 - mine_part
    passed, handed = {}, {}

    def pass_on(d, h):
        ours = piece(d, mine_part, h)
        passed[d, h] = send(ours, ours, gy_prev if h else gy_next)
        handed[d, h] = send(ours, ours, partner)

    def hand_on(d, h):
        theirs = piece(d, other_part, h)
        passed[d, h].wait_recv()
        handed[d, h, 1] = send(theirs, theirs, partner)

    def complete(d):
        for h in range(2):
            handed[d, h].wait_recv()
            handed[d, h, 1].wait_recv()

    arrive(((down, above), (up, below)))
    set_columns(1)
    set_columns(2)
    ring[1, 0].wait_recv()
    ring[2, 0] = send(piece(1, mine_part, 0), piece(2, mine_part, 0), ma_next)
    pass_on(1, 0)
    ring[3, 1].wait_recv()
    ring[2, 1] = send(piece(3, mine_part, 1), piece(2, mine_part, 1), ma_prev)
    pass_on(3, 1)
    for p in range(2):
        arrive(first_beside[p])
    stacked = [cut_and_lend(0, p, at) for p, at in chunks]
    ring[1, 1].wait_recv()
    pass_on(1, 1)
    ring[3, 0].wait_recv()
    pass_on(3, 0)
    for arrivals in stacked:
        arrive(arrivals)
    window(0)
    hand_on(1, 0)
    hand_on(3, 1)
    intensity = add_spectra(0, intensity)
    ring[2, 0].wait_recv()
    pass_on(2, 0)
    ring[2, 1].wait_recv()
    pass_on(2, 1)
    hand_on(1, 1)
    hand_on(3, 0)
    for d in (1, 3):
        complete(d)
        intensity = add_spectra(d, intensity)
    hand_on(2, 0)
    hand_on(2, 1)
    complete(2)
    intensity = add_spectra(2, intensity)

    alpha = None
    for it in range(OUTER):
        backward(live * (intensity - meas[...]), alpha)
        square = combine(it)
        window(it + 1)
        last = it + 1 == OUTER

        def pair(d, change, last=last):
            m = forward_pair(d)
            if not last:
                moved[pair_rows(d), :] = m
            return change + folded(spec[pair_rows(d), :] * m)

        change = 2.0 * lax.fori_loop(0, n_ma, pair, jnp.zeros((kh, n), F32), unroll=True)
        sums = step_size(it, square, squares(live * change))
        next(sums)
        if not last:

            def power(d, total):
                m = moved[pair_rows(d), :]
                return total + folded(m * m)

            moved_power = lax.fori_loop(0, n_ma, power, jnp.zeros((kh, n), F32))
        alpha = next(sums)
        obj[...] += alpha * wide[it + 1, :, :, own_cols]
        if not last:
            intensity = intensity + alpha * (change + alpha * moved_power)
    out_ref[...] = obj[...]
    copies.finish()


def solution(mesh):
    sizes = (mesh.shape["gx"], mesh.shape["gy"], mesh.shape["ma"])

    def shards(object_field, probe_modes, measured, positions, slot_counts):
        n = probe_modes.shape[-1]
        _, tx, ty = object_field.shape
        rim, kh = n // 2, n // 2
        height, width = tx + 2 * rim, ty + 2 * rim
        modes = probe_modes.shape[0] * sizes[2]
        row_chunk = tx // 2
        vmem = pltpu.VMEM
        scratch = [
            vmem((2, tx, ty), F32),
            vmem((OUTER + 1, 2, tx, width), F32),
            vmem((OUTER + 1, 2, height, n), F32),
            vmem((OUTER + 1, 2, 2, tx, n), F32),
            vmem((sizes[2], 2, 2, n, n), F32),
            vmem((kh, n), F32),
            vmem((n, 2 * n), BF16),
            vmem((2 * n, 2 * n), BF16),
            vmem((2 * n, 2 * n), BF16),
            vmem((2 * n, n), BF16),
            vmem((2, n, n), F32),
            vmem((2, 2 * n, n), BF16),
            vmem((n, 2 * n), BF16),
            vmem((modes * kh, 2 * n), F32),
            vmem((modes * kh, 2 * n), F32),
            vmem((2, n, n), BF16),
            vmem((kh, 2 * n), F32),
            vmem((2, n, n), F32),
            vmem((OUTER, 2, height, n), F32),
            vmem((n, 2 * height), BF16),
            vmem((width, 3 * n), BF16),
            vmem((height, 2 * n), BF16),
            vmem((3 * n, width), BF16),
            vmem((3, 8, 128), F32),
            vmem((2 * row_chunk, width), BF16),
            vmem((2 * height, n), BF16),
            vmem((2 * n, n), BF16),
            vmem((2 * row_chunk, 3 * n), BF16),
            vmem((OUTER, 2, tx, width), F32),
            vmem((OUTER, 2, 2, tx, n), F32),
            vmem((OUTER, 2, 2, tx, rim), F32),
            vmem((OUTER, sizes[2] - 1, 4, row_chunk // sizes[2], ty), F32),
            vmem((OUTER, sizes[1] * sizes[2], 1, 128), F32),
            vmem((OUTER, sizes[0], 1, 128), F32),
            pltpu.SemaphoreType.REGULAR((5,)),
            pltpu.SemaphoreType.DMA((4,)),
            pltpu.SemaphoreType.DMA((224,)),
            pltpu.SemaphoreType.DMA((224,)),
        ]
        anywhere = pl.BlockSpec(memory_space=pl.ANY)
        smem = pl.BlockSpec(memory_space=pltpu.SMEM)
        in_vmem = pl.BlockSpec(memory_space=pltpu.VMEM)
        return pl.pallas_call(
            functools.partial(kernel, (*sizes, n, tx, ty)),
            out_shape=jax.ShapeDtypeStruct(object_field.shape, F32),
            in_specs=[anywhere, anywhere, anywhere, smem, smem, in_vmem],
            out_specs=in_vmem,
            scratch_shapes=scratch,
            compiler_params=pltpu.CompilerParams(
                collective_id=0, has_side_effects=True, vmem_limit_bytes=60 * 1024 * 1024
            ),
        )(object_field, probe_modes, measured, positions, slot_counts, jnp.asarray(dft_parts(n)))

    placed = (
        P(None, "gx", "gy"),
        P("ma", None, None, None),
        P("gx", "gy", None, None, None),
        P("gx", "gy", None, None),
        P("gx", "gy"),
    )
    return jax.shard_map(
        shards, mesh=mesh, in_specs=placed, out_specs=P(None, "gx", "gy"), check_vma=False
    )
```

```python
import functools
import math

import jax
import jax.numpy as jnp
import numpy as np
from jax import lax
from jax.experimental import pallas as pl
from jax.experimental.pallas import tpu as pltpu
from jax.sharding import PartitionSpec as P

OUTER = 2
DAMPING = 1.0
CHUNKS = 4
MESH = pl.DeviceIdType.MESH
F32 = jnp.float32
BF16 = jnp.bfloat16


def dft_parts(n):
    ladder = np.arange(n, dtype=np.int32)
    phases = ladder[:, None] * ladder[None, :] % n
    angles = phases.astype(np.float32) * np.float32(2.0 * math.pi / n)
    factor = np.float32(1.0 / math.sqrt(n))
    return np.stack([np.cos(angles) * factor, -np.sin(angles) * factor]).astype(BF16)


class Copies:
    def __init__(self, send_sems, recv_sems):
        self.send_sems, self.recv_sems, self.count, self.pending = send_sems, recv_sems, 0, []

    def make(self, src, dst, device, sends=None):
        copy = pltpu.make_async_remote_copy(
            src_ref=src,
            dst_ref=dst,
            send_sem=self.send_sems.at[self.count],
            recv_sem=self.recv_sems.at[self.count],
            device_id=device,
            device_id_type=MESH,
        )
        self.count += 1
        self.pending.append((copy, sends))
        return copy

    def finish(self):
        for copy, sends in self.pending:
            when(sends, copy.wait_send)
        self.pending = []


def when(condition, action):
    if condition is None:
        action()
    else:
        pl.when(condition)(action)


def kernel(
    dims,
    obj_hbm,
    probe_hbm,
    meas_hbm,
    pos_hbm,
    count_hbm,
    w_hbm,
    out_ref,
    pos_ref,
    count_ref,
    w_ref,
    wide,
    cut,
    lent,
    probes,
    meas,
    t_one,
    t_two,
    t_back,
    t_three,
    win,
    wave,
    half,
    spec,
    moved,
    turned,
    weight,
    patch,
    tall,
    cut_rows,
    cut_cols,
    put_rows,
    put_cols,
    columns,
    terms_cols,
    terms_rows,
    terms_patch,
    terms_put,
    ext,
    from_z,
    from_y,
    from_ma,
    sums_plane,
    sums_line,
    token,
    local_sems,
    send_sems,
    recv_sems,
):
    n_gx, n_gy, n_ma, n, tx, ty = dims
    rim = n // 2
    kh = n // 2
    gx, gy, ma = lax.axis_index("gx"), lax.axis_index("gy"), lax.axis_index("ma")
    core = lax.rem(gx, 2)
    slot, part_k = ma // 2, lax.rem(ma, 2)
    up, down = gx > 0, gx < n_gx - 1
    left, right = gy > 0, gy < n_gy - 1
    copies = Copies(send_sems, recv_sems)
    row_chunk = tx // CHUNKS
    chunks = [(p, j * row_chunk) for p in range(2) for j in range(CHUNKS)]

    barrier = pltpu.get_barrier_semaphore()
    line = [{"gx": lax.rem(gx + o, n_gx)} for o in range(1, n_gx)]
    plane = [
        {"gy": lax.rem(gy + o // n_ma, n_gy), "ma": lax.rem(ma + o % n_ma, n_ma)}
        for o in range(1, n_gy * n_ma)
    ]

    def at_distance(axis, o):
        me, size = {"gx": (gx, n_gx), "gy": (gy, n_gy), "ma": (ma, n_ma)}[axis]
        offsets = {o % size, (size - o) % size}
        return [{axis: lax.rem(me + off, size)} for off in sorted(offsets)]

    def tell(sem, devices):
        for device in devices:
            pl.semaphore_signal(sem, inc=1, device_id=device, device_id_type=MESH)

    nearest = at_distance("gx", 1) + at_distance("gy", 1) + at_distance("ma", 1)
    tell(barrier, nearest)

    k_rows = pl.ds(pl.multiple_of(part_k * kh, kh), kh)
    own_cols = pl.ds(rim, ty)
    table_load = pltpu.make_async_copy(w_hbm, w_ref, local_sems.at[4])
    table_load.start()
    scalar_loads = [
        pltpu.make_async_copy(pos_hbm, pos_ref, local_sems.at[2]),
        pltpu.make_async_copy(count_hbm, count_ref, local_sems.at[5]),
    ]
    for load in scalar_loads:
        load.start()
    loads = [
        pltpu.make_async_copy(obj_hbm, wide.at[0, :, :, own_cols], local_sems.at[0]),
        pltpu.make_async_copy(probe_hbm, probes.at[0], local_sems.at[1]),
        pltpu.make_async_copy(meas_hbm.at[0, 0, slot, k_rows], meas, local_sems.at[3]),
    ]
    for load in loads:
        load.start()
    for load in scalar_loads:
        load.wait()
    row_at, col_at = pos_ref[0, 0, slot, 0], pos_ref[0, 0, slot, 1]
    live = jnp.where(slot < count_ref[0, 0], 1.0, 0.0).astype(F32)
    columns[0] = jnp.full((8, 128), col_at.astype(F32))
    table_load.wait()
    w_re, w_im = w_ref[0], w_ref[1]
    t_two[:n, :n], t_two[:n, n:], t_two[n:, :n], t_two[n:, n:] = w_re, w_im, -w_im, w_re
    t_back[:n, :n], t_back[:n, n:], t_back[n:, :n], t_back[n:, n:] = w_re, -w_im, w_im, w_re
    wk_re, wk_im = w_ref[0, k_rows, :], w_ref[1, k_rows, :]
    t_one[:kh, :n], t_one[:kh, n:], t_one[kh:, :n], t_one[kh:, n:] = wk_re, -wk_im, wk_im, wk_re
    k_cols = pl.ds(pl.multiple_of(part_k * kh, kh), kh)
    wc_re, wc_im = w_ref[0, :, k_cols], w_ref[1, :, k_cols]
    t_three[:n, :kh], t_three[:n, kh:] = wc_re, wc_im
    t_three[n:, :kh], t_three[n:, kh:] = -wc_im, wc_re

    def clear(ref):
        ref[...] = jnp.zeros(ref.shape, ref.dtype)

    for it in range(OUTER + 1):
        for p in range(2):
            when(gx == 0, functools.partial(clear, cut.at[it, p, pl.ds(0, rim)]))
            when(gx == n_gx - 1, functools.partial(clear, cut.at[it, p, pl.ds(rim + tx, rim)]))
            when(gy == 0, functools.partial(clear, wide.at[it, p, :, pl.ds(0, rim)]))
            when(gy == n_gy - 1, functools.partial(clear, wide.at[it, p, :, pl.ds(rim + ty, rim)]))
            if it < OUTER:
                when(gx == n_gx - 1, functools.partial(clear, from_z.at[it, 0, p]))
                when(gx == 0, functools.partial(clear, from_z.at[it, 1, p]))
                when(gy == n_gy - 1, functools.partial(clear, from_y.at[it, 0, p]))
                when(gy == 0, functools.partial(clear, from_y.at[it, 1, p]))
    when(gx == 0, functools.partial(clear, columns.at[1]))
    when(gx == n_gx - 1, functools.partial(clear, columns.at[2]))

    height, width = 2 * rim + tx, 2 * rim + ty

    def chosen(shape, dim, first):
        here = lax.broadcasted_iota(jnp.int32, shape, dim)
        there = lax.broadcasted_iota(jnp.int32, shape, 1 - dim)
        return jnp.where((here - there).astype(F32) == first, 1.0, 0.0).astype(BF16)

    row_first = jnp.full((1, 1), row_at.astype(F32))
    for i in range(2):
        cut_rows[:, i * height : (i + 1) * height] = chosen((n, height), 1, row_first)
        put_rows[:, i * n : (i + 1) * n] = chosen((height, n), 0, row_first)

    def set_columns(which):
        first = columns[which][:1, :1]
        cut_cols[:, which * n : (which + 1) * n] = chosen((width, n), 0, first)
        put_cols[which * n : (which + 1) * n] = chosen((n, width), 1, first)

    set_columns(0)

    for load in loads:
        load.wait()
    pl.semaphore_wait(barrier, len(nearest))

    ma_next, ma_prev = {"ma": lax.rem(ma + 1, n_ma)}, {"ma": lax.rem(ma + n_ma - 1, n_ma)}
    gy_next, gy_prev = {"gy": lax.rem(gy + 1, n_gy)}, {"gy": lax.rem(gy + n_gy - 1, n_gy)}
    partner = {"gx": gx + 1 - 2 * core}
    mine_part = lax.rem(gy, 2)
    halves = (pl.ds(0, kh), pl.ds(kh, kh))

    def piece(d, part, h):
        return probes.at[d, core, part, halves[h]]

    def send(src, dst, device):
        copy = copies.make(src, dst, device)
        copy.start()
        return copy

    ring = {}
    for h, g in ((0, 1), (1, 0)):
        ring[1, h] = send(piece(0, mine_part, h), piece(1, mine_part, h), ma_next)
        ring[3, g] = send(piece(0, mine_part, g), piece(3, mine_part, g), ma_prev)

    above = copies.make(columns.at[0], columns.at[2], {"gx": gx - 1}, up)
    below = copies.make(columns.at[0], columns.at[1], {"gx": gx + 1}, down)
    when(up, above.start)
    when(down, below.start)

    def exchange(condition_low, condition_high, axis, me, low, high):
        first = copies.make(*low, {axis: me - 1}, condition_low)
        second = copies.make(*high, {axis: me + 1}, condition_high)
        when(condition_low, first.start)
        when(condition_high, second.start)
        return ((condition_high, first), (condition_low, second))

    def arrive(arrivals):
        for condition, copy in arrivals:
            when(condition, copy.wait_recv)

    def beside(buf, p, at, rows):
        strip = buf.at[p, pl.ds(at, rows)]
        return exchange(
            left,
            right,
            "gy",
            gy,
            (strip.at[:, pl.ds(rim, rim)], strip.at[:, pl.ds(rim + ty, rim)]),
            (strip.at[:, pl.ds(ty, rim)], strip.at[:, pl.ds(0, rim)]),
        )

    first_beside = [beside(wide.at[0], p, 0, tx) for p in range(2)]

    tell(token.at[0], at_distance("gx", 1))
    tell(token.at[3], at_distance("gy", 1) + at_distance("ma", 1))
    pl.semaphore_wait(token.at[0], 2)
    tell(token.at[1], at_distance("gx", 2))
    pl.semaphore_wait(token.at[3], 4)
    tell(token.at[4], at_distance("gy", 2) + at_distance("ma", 2))
    pl.semaphore_wait(token.at[1], 2)
    tell(token.at[2], at_distance("gx", 4))
    pl.semaphore_wait(token.at[4], 2)
    pl.semaphore_wait(token.at[2], 2)


    def two_terms(x, ref, at, axis):
        top = x.astype(BF16)
        rest = (x - top.astype(F32)).astype(BF16)
        size = x.shape[axis]
        if axis == 0:
            ref[at : at + size], ref[at + size : at + 2 * size] = top, rest
        else:
            ref[:, at : at + size], ref[:, at + size : at + 2 * size] = top, rest

    def dot(x, y):
        return jnp.dot(x, y, preferred_element_type=F32)

    def stack(x, ref, at):
        rows, cols = x.shape
        top = x.astype(BF16)
        ref[:rows, at : at + cols] = top
        ref[rows:, at : at + cols] = (x - top.astype(F32)).astype(BF16)

    def both(x):
        rows = x.shape[0] // 2
        return x[:rows] + x[rows:]

    def cut_and_lend(it, p, at):
        rows = pl.ds(at, row_chunk)
        stack(wide[it, p, rows], terms_cols, 0)
        x = both(dot(terms_cols[...], cut_cols[...]))
        cut[it, p, pl.ds(rim + at, row_chunk)] = x[:, :n]
        lent[it, 0, p, rows] = x[:, n : 2 * n]
        lent[it, 1, p, rows] = x[:, 2 * n :]
        return exchange(
            up,
            down,
            "gx",
            gx,
            (lent.at[it, 0, p, rows], cut.at[it, p, pl.ds(rim + tx + at, row_chunk)]),
            (lent.at[it, 1, p, rows], cut.at[it, p, pl.ds(at, row_chunk)]),
        )

    def window(it):
        def part(p, _):
            two_terms(cut[it, p], terms_rows, 0, 0)
            win[p] = dot(cut_rows[...], terms_rows[...])
            return 0

        lax.fori_loop(0, 2, part, 0)

    def forward_pair(d):
        for c in range(2):
            pr, pi = probes[d, c, 0], probes[d, c, 1]
            wr, wi = win[0], win[1]
            wave[c, :n] = (pr * wr - pi * wi).astype(BF16)
            wave[c, n:] = (pr * wi + pi * wr).astype(BF16)
            h = dot(t_one[...], wave[c]).astype(BF16)
            half[c * kh : (c + 1) * kh, :n] = h[:kh]
            half[c * kh : (c + 1) * kh, n:] = h[kh:]
        return dot(half[...], t_two[...])

    def pair_rows(d):
        return pl.ds(pl.multiple_of(d * n, n), n)

    def folded(x):
        x = x[:kh] + x[kh:]
        return x[:, :n] + x[:, n:]

    def backward(misfit, alpha):
        weight[:, :n] = 2.0 * misfit
        weight[:, n:] = 2.0 * misfit

        def pair(d, _):
            y = weight[...]
            f = spec[pair_rows(d), :]
            if alpha is not None:
                f = f + alpha * moved[pair_rows(d), :]
                spec[pair_rows(d), :] = f
            half[:kh] = (f[:kh] * y).astype(BF16)
            half[kh:] = (f[kh:] * y).astype(BF16)
            b = dot(half[...], t_back[...]).astype(BF16)
            for c in range(2):
                turned[c, :kh] = b[c * kh : (c + 1) * kh, :n]
                turned[c, kh:] = b[c * kh : (c + 1) * kh, n:]
                g = dot(t_three[...], turned[c])
                pr, pi = probes[d, c, 0], probes[d, c, 1]
                patch[0] += pr * g[:n] + pi * g[n:]
                patch[1] += pr * g[n:] - pi * g[:n]
            return 0

        clear(patch)
        lax.fori_loop(0, n_ma, pair, 0, unroll=True)

    def place(it):
        def part(p, _):
            two_terms(patch[p], terms_patch, 0, 0)
            tall[it, p] = dot(put_rows[...], terms_patch[...])
            return 0

        lax.fori_loop(0, 2, part, 0)

    def combine(it):
        place(it)
        folds = []
        for p, at in chunks:
            rows = pl.ds(at, row_chunk)
            folds.append(
                exchange(
                    up,
                    down,
                    "gx",
                    gx,
                    (tall.at[it, p, rows], from_z.at[it, 0, p, rows]),
                    (tall.at[it, p, pl.ds(rim + tx + at, row_chunk)], from_z.at[it, 1, p, rows]),
                )
            )
        sides = []
        for i, (p, at) in enumerate(chunks):
            rows = pl.ds(at, row_chunk)
            arrive(folds[i])
            stack(tall[it, p, pl.ds(rim + at, row_chunk)], terms_put, 0)
            stack(from_z[it, 1, p, rows], terms_put, n)
            stack(from_z[it, 0, p, rows], terms_put, 2 * n)
            ext[it, p, rows] = both(dot(terms_put[...], put_cols[...]))
            strip = ext.at[it, p, rows]
            sides.append(
                exchange(
                    left,
                    right,
                    "gy",
                    gy,
                    (strip.at[:, pl.ds(0, rim)], from_y.at[it, 0, p, rows]),
                    (strip.at[:, pl.ds(rim + ty, rim)], from_y.at[it, 1, p, rows]),
                )
            )
        share = row_chunk // n_ma
        parts = []
        for i, (p, at) in enumerate(chunks):
            rows = pl.ds(at, row_chunk)
            arrive(sides[i])
            ext[it, p, rows, pl.ds(ty, rim)] += from_y[it, 0, p, rows]
            ext[it, p, rows, pl.ds(rim, rim)] += from_y[it, 1, p, rows]
            batch = []
            for o in range(1, n_ma):
                peer = lax.rem(ma + o, n_ma)
                theirs = pl.ds(pl.multiple_of(at + peer * share, share), share)
                copy = copies.make(
                    ext.at[it, p, theirs, own_cols], from_ma.at[it, o - 1, i], {"ma": peer}
                )
                copy.start()
                batch.append(copy)
            parts.append(batch)
        gathers, square = [], jnp.zeros((8, 128), F32)
        for i, (p, at) in enumerate(chunks):
            mine = pl.ds(pl.multiple_of(at + ma * share, share), share)
            total = ext[it, p, mine, own_cols]
            for o in range(1, n_ma):
                parts[i][o - 1].wait_recv()
                total += from_ma[it, o - 1, i]
            wide[it + 1, p, mine, own_cols] = -total
            square += squares(total)
            batch = []
            for o in range(1, n_ma):
                ours = wide.at[it + 1, p, mine, own_cols]
                copy = copies.make(ours, ours, {"ma": lax.rem(ma + o, n_ma)})
                copy.start()
                batch.append(copy)
            gathers.append(batch)
        sides = []
        for i, (p, at) in enumerate(chunks):
            for copy in gathers[i]:
                copy.wait_recv()
            sides.append(beside(wide.at[it + 1], p, at, row_chunk))
        stacked = []
        for i, (p, at) in enumerate(chunks):
            arrive(sides[i])
            stacked.append(cut_and_lend(it + 1, p, at))
        for arrivals in stacked:
            arrive(arrivals)
        return square

    def squares(x):
        x = x * x
        out = x[:, :128]
        for i in range(1, x.shape[1] // 128):
            out = out + x[:, i * 128 : (i + 1) * 128]
        return jnp.sum(out.reshape(-1, 8, 128), axis=0)

    def row_of(x):
        x = jnp.sum(x, axis=0, keepdims=True)
        return x + pltpu.roll(x, 64, 1)

    def step_size(it, square, changes):
        lane = lax.broadcasted_iota(jnp.int32, (1, 128), 1)
        value = jnp.where(lane < 64, row_of(square), row_of(changes))
        for buf, me, devices in (
            (sums_plane, gy * n_ma + ma, plane),
            (sums_line, gx, line),
        ):
            buf[it, me] = value
            mine = buf.at[it, me]
            batch = [send(mine, mine, device) for device in devices]
            if devices is plane:
                yield
            for copy in batch:
                copy.wait_recv()
            value = buf[it, 0]
            for i in range(1, len(devices) + 1):
                value += buf[it, i]
        norm = jnp.sum(jnp.where(lane < 64, value, 0.0), keepdims=True)
        change = jnp.sum(jnp.where(lane < 64, 0.0, value), keepdims=True)
        yield norm / (change + DAMPING * norm)

    intensity = jnp.zeros((kh, n), F32)

    def add_spectra(d, total):
        f = forward_pair(d)
        spec[pair_rows(d), :] = f
        return total + folded(f * f)

    other_part = 1 - mine_part
    passed, handed = {}, {}

    def pass_on(d, h):
        ours = piece(d, mine_part, h)
        passed[d, h] = send(ours, ours, gy_prev if h else gy_next)
        handed[d, h] = send(ours, ours, partner)

    def hand_on(d, h):
        theirs = piece(d, other_part, h)
        passed[d, h].wait_recv()
        handed[d, h, 1] = send(theirs, theirs, partner)

    def complete(d):
        for h in range(2):
            handed[d, h].wait_recv()
            handed[d, h, 1].wait_recv()

    arrive(((down, above), (up, below)))
    set_columns(1)
    set_columns(2)
    ring[1, 0].wait_recv()
    ring[2, 0] = send(piece(1, mine_part, 0), piece(2, mine_part, 0), ma_next)
    pass_on(1, 0)
    ring[3, 1].wait_recv()
    ring[2, 1] = send(piece(3, mine_part, 1), piece(2, mine_part, 1), ma_prev)
    pass_on(3, 1)
    for p in range(2):
        arrive(first_beside[p])
    stacked = [cut_and_lend(0, p, at) for p, at in chunks]
    ring[1, 1].wait_recv()
    pass_on(1, 1)
    ring[3, 0].wait_recv()
    pass_on(3, 0)
    hand_on(1, 0)
    hand_on(3, 1)
    ring[2, 0].wait_recv()
    pass_on(2, 0)
    ring[2, 1].wait_recv()
    pass_on(2, 1)
    for arrivals in stacked:
        arrive(arrivals)
    window(0)
    hand_on(1, 1)
    hand_on(3, 0)
    intensity = add_spectra(0, intensity)
    complete(1)
    intensity = add_spectra(1, intensity)
    hand_on(2, 0)
    hand_on(2, 1)
    complete(3)
    intensity = add_spectra(3, intensity)
    complete(2)
    intensity = add_spectra(2, intensity)

    alpha = None
    for it in range(OUTER):
        backward(live * (intensity - meas[...]), alpha)
        square = combine(it)
        window(it + 1)
        last = it + 1 == OUTER

        def pair(d, change, last=last):
            m = forward_pair(d)
            if not last:
                moved[pair_rows(d), :] = m
            return change + folded(spec[pair_rows(d), :] * m)

        change = 2.0 * lax.fori_loop(0, n_ma, pair, jnp.zeros((kh, n), F32), unroll=True)
        sums = step_size(it, square, squares(live * change))
        next(sums)
        if not last:

            def power(d, total):
                m = moved[pair_rows(d), :]
                return total + folded(m * m)

            moved_power = lax.fori_loop(0, n_ma, power, jnp.zeros((kh, n), F32))
        alpha = next(sums)
        step = alpha * wide[it + 1, :, :, own_cols]
        out_ref[...] = step if it == 0 else out_ref[...] + step
        if not last:
            intensity = intensity + alpha * (change + alpha * moved_power)
    copies.finish()


def solution(mesh):
    sizes = (mesh.shape["gx"], mesh.shape["gy"], mesh.shape["ma"])

    def shards(object_field, probe_modes, measured, positions, slot_counts):
        n = probe_modes.shape[-1]
        _, tx, ty = object_field.shape
        rim, kh = n // 2, n // 2
        height, width = tx + 2 * rim, ty + 2 * rim
        modes = probe_modes.shape[0] * sizes[2]
        row_chunk = tx // CHUNKS
        vmem = pltpu.VMEM
        scratch = [
            pltpu.SMEM(positions.shape, jnp.int32),
            pltpu.SMEM(slot_counts.shape, jnp.int32),
            vmem((2, n, n), BF16),
            vmem((OUTER + 1, 2, tx, width), F32),
            vmem((OUTER + 1, 2, height, n), F32),
            vmem((OUTER + 1, 2, 2, tx, n), F32),
            vmem((sizes[2], 2, 2, n, n), F32),
            vmem((kh, n), F32),
            vmem((n, 2 * n), BF16),
            vmem((2 * n, 2 * n), BF16),
            vmem((2 * n, 2 * n), BF16),
            vmem((2 * n, n), BF16),
            vmem((2, n, n), F32),
            vmem((2, 2 * n, n), BF16),
            vmem((n, 2 * n), BF16),
            vmem((modes * kh, 2 * n), F32),
            vmem((modes * kh, 2 * n), F32),
            vmem((2, n, n), BF16),
            vmem((kh, 2 * n), F32),
            vmem((2, n, n), F32),
            vmem((OUTER, 2, height, n), F32),
            vmem((n, 2 * height), BF16),
            vmem((width, 3 * n), BF16),
            vmem((height, 2 * n), BF16),
            vmem((3 * n, width), BF16),
            vmem((3, 8, 128), F32),
            vmem((2 * row_chunk, width), BF16),
            vmem((2 * height, n), BF16),
            vmem((2 * n, n), BF16),
            vmem((2 * row_chunk, 3 * n), BF16),
            vmem((OUTER, 2, tx, width), F32),
            vmem((OUTER, 2, 2, tx, n), F32),
            vmem((OUTER, 2, 2, tx, rim), F32),
            vmem((OUTER, sizes[2] - 1, 2 * CHUNKS, row_chunk // sizes[2], ty), F32),
            vmem((OUTER, sizes[1] * sizes[2], 1, 128), F32),
            vmem((OUTER, sizes[0], 1, 128), F32),
            pltpu.SemaphoreType.REGULAR((5,)),
            pltpu.SemaphoreType.DMA((6,)),
            pltpu.SemaphoreType.DMA((112 + 56 * CHUNKS,)),
            pltpu.SemaphoreType.DMA((112 + 56 * CHUNKS,)),
        ]
        anywhere = pl.BlockSpec(memory_space=pl.ANY)
        in_vmem = pl.BlockSpec(memory_space=pltpu.VMEM)
        update = pl.pallas_call(
            functools.partial(kernel, (*sizes, n, tx, ty)),
            out_shape=pltpu.VMEM(object_field.shape, F32),
            in_specs=[anywhere] * 6,
            out_specs=in_vmem,
            scratch_shapes=scratch,
            compiler_params=pltpu.CompilerParams(
                collective_id=0, has_side_effects=True, vmem_limit_bytes=60 * 1024 * 1024
            ),
        )(object_field, probe_modes, measured, positions, slot_counts, jnp.asarray(dft_parts(n)))
        return object_field + update

    placed = (
        P(None, "gx", "gy"),
        P("ma", None, None, None),
        P("gx", "gy", None, None, None),
        P("gx", "gy", None, None),
        P("gx", "gy"),
    )
    return jax.shard_map(
        shards, mesh=mesh, in_specs=placed, out_specs=P(None, "gx", "gy"), check_vma=False
    )
```

```python
import functools
import math

import jax
import jax.numpy as jnp
import numpy as np
from jax import lax
from jax.experimental import pallas as pl
from jax.experimental.pallas import tpu as pltpu
from jax.sharding import PartitionSpec as P

OUTER = 2
DAMPING = 1.0
PIECES = 4
GROUP = 4
CHUNKS = 4
MESH = pl.DeviceIdType.MESH
F32 = jnp.float32
BF16 = jnp.bfloat16


def dft_parts(n):
    ladder = np.arange(n, dtype=np.int32)
    phases = ladder[:, None] * ladder[None, :] % n
    angles = phases.astype(np.float32) * np.float32(2.0 * math.pi / n)
    factor = np.float32(1.0 / math.sqrt(n))
    return np.stack([np.cos(angles) * factor, -np.sin(angles) * factor]).astype(BF16)


class Copies:
    def __init__(self, send_sems, recv_sems):
        self.send_sems, self.recv_sems, self.count, self.pending = send_sems, recv_sems, 0, []

    def make(self, src, dst, device, sends=None):
        copy = pltpu.make_async_remote_copy(
            src_ref=src,
            dst_ref=dst,
            send_sem=self.send_sems.at[self.count],
            recv_sem=self.recv_sems.at[self.count],
            device_id=device,
            device_id_type=MESH,
        )
        self.count += 1
        self.pending.append((copy, sends))
        return copy

    def finish(self):
        for copy, sends in self.pending:
            when(sends, copy.wait_send)
        self.pending = []


def when(condition, action):
    if condition is None:
        action()
    else:
        pl.when(condition)(action)


def kernel(
    dims,
    obj_hbm,
    probe_hbm,
    meas_hbm,
    pos_hbm,
    count_hbm,
    w_hbm,
    out_ref,
    pos_ref,
    count_ref,
    w_ref,
    wide,
    cut,
    lent,
    probes,
    meas,
    t_one,
    t_two,
    t_back,
    t_three,
    win,
    wave,
    half,
    spec,
    moved,
    turned,
    weight,
    patch,
    tall,
    cut_rows,
    cut_cols,
    put_rows,
    put_cols,
    columns,
    terms_cols,
    terms_rows,
    terms_patch,
    terms_put,
    terms_own,
    ext,
    from_z,
    from_y,
    from_ma,
    sums_plane,
    sums_line,
    token,
    local_sems,
    send_sems,
    recv_sems,
):
    n_gx, n_gy, n_ma, n, tx, ty = dims
    rim = n // 2
    kh = n // 2
    gx, gy, ma = lax.axis_index("gx"), lax.axis_index("gy"), lax.axis_index("ma")
    core = lax.rem(gx, 2)
    slot, part_k = ma // 2, lax.rem(ma, 2)
    up, down = gx > 0, gx < n_gx - 1
    left, right = gy > 0, gy < n_gy - 1
    copies = Copies(send_sems, recv_sems)
    row_chunk = tx // CHUNKS
    chunks = [(p, j * row_chunk) for p in range(2) for j in range(CHUNKS)]

    barrier = pltpu.get_barrier_semaphore()
    line = [{"gx": lax.rem(gx + o, n_gx)} for o in range(1, n_gx)]
    plane = [
        {"gy": lax.rem(gy + o // n_ma, n_gy), "ma": lax.rem(ma + o % n_ma, n_ma)}
        for o in range(1, n_gy * n_ma)
    ]

    def at_distance(axis, o):
        me, size = {"gx": (gx, n_gx), "gy": (gy, n_gy), "ma": (ma, n_ma)}[axis]
        offsets = {o % size, (size - o) % size}
        return [{axis: lax.rem(me + off, size)} for off in sorted(offsets)]

    def tell(sem, devices):
        for device in devices:
            pl.semaphore_signal(sem, inc=1, device_id=device, device_id_type=MESH)

    nearest = at_distance("gx", 1) + at_distance("gy", 1) + at_distance("ma", 1)
    tell(barrier, nearest)

    k_rows = pl.ds(pl.multiple_of(part_k * kh, kh), kh)
    own_cols = pl.ds(rim, ty)
    table_load = pltpu.make_async_copy(w_hbm, w_ref, local_sems.at[4])
    table_load.start()
    scalar_loads = [
        pltpu.make_async_copy(pos_hbm, pos_ref, local_sems.at[2]),
        pltpu.make_async_copy(count_hbm, count_ref, local_sems.at[5]),
    ]
    for load in scalar_loads:
        load.start()
    loads = [
        pltpu.make_async_copy(obj_hbm, wide.at[0, :, :, own_cols], local_sems.at[0]),
        pltpu.make_async_copy(probe_hbm, probes.at[0], local_sems.at[1]),
        pltpu.make_async_copy(meas_hbm.at[0, 0, slot, k_rows], meas, local_sems.at[3]),
    ]
    for load in loads:
        load.start()
    for load in scalar_loads:
        load.wait()
    row_at, col_at = pos_ref[0, 0, slot, 0], pos_ref[0, 0, slot, 1]
    live = jnp.where(slot < count_ref[0, 0], 1.0, 0.0).astype(F32)
    columns[0] = jnp.full((8, 128), col_at.astype(F32))
    table_load.wait()
    w_re, w_im = w_ref[0], w_ref[1]
    t_two[:n, :n], t_two[:n, n:], t_two[n:, :n], t_two[n:, n:] = w_re, w_im, -w_im, w_re
    t_back[:n, :n], t_back[:n, n:], t_back[n:, :n], t_back[n:, n:] = w_re, -w_im, w_im, w_re
    wk_re, wk_im = w_ref[0, k_rows, :], w_ref[1, k_rows, :]
    t_one[:kh, :n], t_one[:kh, n:], t_one[kh:, :n], t_one[kh:, n:] = wk_re, -wk_im, wk_im, wk_re
    k_cols = pl.ds(pl.multiple_of(part_k * kh, kh), kh)
    wc_re, wc_im = w_ref[0, :, k_cols], w_ref[1, :, k_cols]
    t_three[:n, :kh], t_three[:n, kh:] = wc_re, wc_im
    t_three[n:, :kh], t_three[n:, kh:] = -wc_im, wc_re

    def clear(ref):
        ref[...] = jnp.zeros(ref.shape, ref.dtype)

    for it in range(OUTER + 1):
        for p in range(2):
            when(gx == 0, functools.partial(clear, cut.at[it, p, pl.ds(0, rim)]))
            when(gx == n_gx - 1, functools.partial(clear, cut.at[it, p, pl.ds(rim + tx, rim)]))
            when(gy == 0, functools.partial(clear, wide.at[it, p, :, pl.ds(0, rim)]))
            when(gy == n_gy - 1, functools.partial(clear, wide.at[it, p, :, pl.ds(rim + ty, rim)]))
            if it < OUTER:
                when(gx == n_gx - 1, functools.partial(clear, from_z.at[it, 0, p]))
                when(gx == 0, functools.partial(clear, from_z.at[it, 1, p]))
                when(gy == n_gy - 1, functools.partial(clear, from_y.at[it, 0, p]))
                when(gy == 0, functools.partial(clear, from_y.at[it, 1, p]))
    when(gx == 0, functools.partial(clear, columns.at[1]))
    when(gx == n_gx - 1, functools.partial(clear, columns.at[2]))

    height, width = 2 * rim + tx, 2 * rim + ty

    def chosen(shape, dim, first):
        here = lax.broadcasted_iota(jnp.int32, shape, dim)
        there = lax.broadcasted_iota(jnp.int32, shape, 1 - dim)
        return jnp.where((here - there).astype(F32) == first, 1.0, 0.0).astype(BF16)

    row_first = jnp.full((1, 1), row_at.astype(F32))
    for i in range(2):
        cut_rows[:, i * height : (i + 1) * height] = chosen((n, height), 1, row_first)
        put_rows[:, i * n : (i + 1) * n] = chosen((height, n), 0, row_first)

    def set_columns(which):
        first = columns[which][:1, :1]
        cut_cols[:, which * n : (which + 1) * n] = chosen((width, n), 0, first)
        put_cols[which * n : (which + 1) * n] = chosen((n, width), 1, first)

    set_columns(0)

    for load in loads:
        load.wait()
    pl.semaphore_wait(barrier, len(nearest))

    ma_next, ma_prev = {"ma": lax.rem(ma + 1, n_ma)}, {"ma": lax.rem(ma + n_ma - 1, n_ma)}
    gy_next, gy_prev = {"gy": lax.rem(gy + 1, n_gy)}, {"gy": lax.rem(gy + n_gy - 1, n_gy)}
    partner = {"gx": gx + 1 - 2 * core}
    mine_part = lax.rem(gy, 2)
    step = n // PIECES

    def piece(d, part, h):
        return probes.at[d, core, part, pl.ds(h * step, step)]

    def send(src, dst, device):
        copy = copies.make(src, dst, device)
        copy.start()
        return copy

    ring = {}
    for h in range(PIECES):
        g = PIECES - 1 - h
        ring[1, h] = send(piece(0, mine_part, h), piece(1, mine_part, h), ma_next)
        ring[3, g] = send(piece(0, mine_part, g), piece(3, mine_part, g), ma_prev)

    above = copies.make(columns.at[0], columns.at[2], {"gx": gx - 1}, up)
    below = copies.make(columns.at[0], columns.at[1], {"gx": gx + 1}, down)
    when(up, above.start)
    when(down, below.start)

    def exchange(condition_low, condition_high, axis, me, low, high):
        first = copies.make(*low, {axis: me - 1}, condition_low)
        second = copies.make(*high, {axis: me + 1}, condition_high)
        when(condition_low, first.start)
        when(condition_high, second.start)
        return ((condition_high, first), (condition_low, second))

    def arrive(arrivals):
        for condition, copy in arrivals:
            when(condition, copy.wait_recv)

    def beside(buf, p, at, rows):
        strip = buf.at[p, pl.ds(at, rows)]
        return exchange(
            left,
            right,
            "gy",
            gy,
            (strip.at[:, pl.ds(rim, rim)], strip.at[:, pl.ds(rim + ty, rim)]),
            (strip.at[:, pl.ds(ty, rim)], strip.at[:, pl.ds(0, rim)]),
        )

    first_beside = [beside(wide.at[0], p, 0, tx) for p in range(2)]

    tell(token.at[0], at_distance("gx", 1))
    tell(token.at[3], at_distance("gy", 1) + at_distance("ma", 1))
    pl.semaphore_wait(token.at[0], 2)
    tell(token.at[1], at_distance("gx", 2))
    pl.semaphore_wait(token.at[3], 4)
    tell(token.at[4], at_distance("gy", 2) + at_distance("ma", 2))
    pl.semaphore_wait(token.at[1], 2)
    tell(token.at[2], at_distance("gx", 4))
    pl.semaphore_wait(token.at[4], 2)
    pl.semaphore_wait(token.at[2], 2)


    def two_terms(x, ref, at, axis):
        top = x.astype(BF16)
        rest = (x - top.astype(F32)).astype(BF16)
        size = x.shape[axis]
        if axis == 0:
            ref[at : at + size], ref[at + size : at + 2 * size] = top, rest
        else:
            ref[:, at : at + size], ref[:, at + size : at + 2 * size] = top, rest

    def dot(x, y):
        return jnp.dot(x, y, preferred_element_type=F32)

    def stack(x, ref, at):
        rows, cols = x.shape
        top = x.astype(BF16)
        ref[:rows, at : at + cols] = top
        ref[rows:, at : at + cols] = (x - top.astype(F32)).astype(BF16)

    def both(x):
        rows = x.shape[0] // 2
        return x[:rows] + x[rows:]

    def lend(it, p, at, count):
        rows = pl.ds(at, count)
        stack(wide[it, p, rows], terms_cols.at[: 2 * count], 0)
        x = both(dot(terms_cols[: 2 * count], cut_cols[:, n:]))
        lent[it, 0, p, rows] = x[:, :n]
        lent[it, 1, p, rows] = x[:, n:]
        return exchange(
            up,
            down,
            "gx",
            gx,
            (lent.at[it, 0, p, rows], cut.at[it, p, pl.ds(rim + tx + at, count)]),
            (lent.at[it, 1, p, rows], cut.at[it, p, pl.ds(at, count)]),
        )

    def keep(it, p):
        stack(wide[it, p], terms_cols, 0)
        cut[it, p, pl.ds(rim, tx)] = both(dot(terms_cols[...], cut_cols[:, :n]))

    def window(it):
        def part(p, _):
            two_terms(cut[it, p], terms_rows, 0, 0)
            win[p] = dot(cut_rows[...], terms_rows[...])
            return 0

        lax.fori_loop(0, 2, part, 0)

    def group_rows(first, count):
        return pl.ds(pl.multiple_of(first * n, n), count * n)

    def forward(first, count):
        for c in range(2 * count):
            d = first + c // 2
            pr, pi = probes[d, c % 2, 0], probes[d, c % 2, 1]
            wr, wi = win[0], win[1]
            wave[c, :n] = (pr * wr - pi * wi).astype(BF16)
            wave[c, n:] = (pr * wi + pi * wr).astype(BF16)
            h = dot(t_one[...], wave[c]).astype(BF16)
            half[c * kh : (c + 1) * kh, :n] = h[:kh]
            half[c * kh : (c + 1) * kh, n:] = h[kh:]
        return dot(half[: count * n], t_two[...])

    def folded(x):
        total = x[:kh]
        for i in range(1, x.shape[0] // kh):
            total = total + x[i * kh : (i + 1) * kh]
        return total[:, :n] + total[:, n:]

    def backward(misfit, alpha):
        weight[:, :n] = 2.0 * misfit
        weight[:, n:] = 2.0 * misfit

        def group(i, _):
            first = i * GROUP
            y = weight[...]
            f = spec[group_rows(first, GROUP), :]
            if alpha is not None:
                f = f + alpha * moved[group_rows(first, GROUP), :]
                spec[group_rows(first, GROUP), :] = f
            for c in range(2 * GROUP):
                half[c * kh : (c + 1) * kh] = (f[c * kh : (c + 1) * kh] * y).astype(BF16)
            b = dot(half[...], t_back[...]).astype(BF16)
            for c in range(2 * GROUP):
                turned[c, :kh] = b[c * kh : (c + 1) * kh, :n]
                turned[c, kh:] = b[c * kh : (c + 1) * kh, n:]
                g = dot(t_three[...], turned[c])
                d = first + c // 2
                pr, pi = probes[d, c % 2, 0], probes[d, c % 2, 1]
                patch[0] += pr * g[:n] + pi * g[n:]
                patch[1] += pr * g[n:] - pi * g[:n]
            return 0

        clear(patch)
        lax.fori_loop(0, n_ma // GROUP, group, 0, unroll=True)

    def place(it):
        def part(p, _):
            two_terms(patch[p], terms_patch, 0, 0)
            tall[it, p] = dot(put_rows[...], terms_patch[...])
            return 0

        lax.fori_loop(0, 2, part, 0)

    def combine(it):
        place(it)
        folds = []
        for p, at in chunks:
            rows = pl.ds(at, row_chunk)
            folds.append(
                exchange(
                    up,
                    down,
                    "gx",
                    gx,
                    (tall.at[it, p, rows], from_z.at[it, 0, p, rows]),
                    (tall.at[it, p, pl.ds(rim + tx + at, row_chunk)], from_z.at[it, 1, p, rows]),
                )
            )
        for p in range(2):
            stack(tall[it, p, pl.ds(rim, tx)], terms_own, 0)
            ext[it, p] = both(dot(terms_own[...], put_cols[:n]))
        sides = []
        for i, (p, at) in enumerate(chunks):
            rows = pl.ds(at, row_chunk)
            arrive(folds[i])
            stack(from_z[it, 1, p, rows], terms_put, 0)
            stack(from_z[it, 0, p, rows], terms_put, n)
            ext[it, p, rows] += both(dot(terms_put[...], put_cols[n:]))
            strip = ext.at[it, p, rows]
            sides.append(
                exchange(
                    left,
                    right,
                    "gy",
                    gy,
                    (strip.at[:, pl.ds(0, rim)], from_y.at[it, 0, p, rows]),
                    (strip.at[:, pl.ds(rim + ty, rim)], from_y.at[it, 1, p, rows]),
                )
            )
        share = row_chunk // n_ma
        parts = []
        for i, (p, at) in enumerate(chunks):
            rows = pl.ds(at, row_chunk)
            arrive(sides[i])
            ext[it, p, rows, pl.ds(ty, rim)] += from_y[it, 0, p, rows]
            ext[it, p, rows, pl.ds(rim, rim)] += from_y[it, 1, p, rows]
            batch = []
            for o in range(1, n_ma):
                peer = lax.rem(ma + o, n_ma)
                theirs = pl.ds(pl.multiple_of(at + peer * share, share), share)
                copy = copies.make(
                    ext.at[it, p, theirs, own_cols], from_ma.at[it, o - 1, i], {"ma": peer}
                )
                copy.start()
                batch.append(copy)
            parts.append(batch)
        gathers, square = [], jnp.zeros((8, 128), F32)
        for i, (p, at) in enumerate(chunks):
            mine = pl.ds(pl.multiple_of(at + ma * share, share), share)
            total = ext[it, p, mine, own_cols]
            for o in range(1, n_ma):
                parts[i][o - 1].wait_recv()
                total += from_ma[it, o - 1, i]
            wide[it + 1, p, mine, own_cols] = -total
            square += squares(total)
            batch = []
            for o in range(1, n_ma):
                ours = wide.at[it + 1, p, mine, own_cols]
                copy = copies.make(ours, ours, {"ma": lax.rem(ma + o, n_ma)})
                copy.start()
                batch.append(copy)
            gathers.append(batch)
        sides = []
        for i, (p, at) in enumerate(chunks):
            for copy in gathers[i]:
                copy.wait_recv()
            sides.append(beside(wide.at[it + 1], p, at, row_chunk))
        stacked = []
        for i, (p, at) in enumerate(chunks):
            arrive(sides[i])
            stacked.append(lend(it + 1, p, at, row_chunk))
        for p in range(2):
            keep(it + 1, p)
        for arrivals in stacked:
            arrive(arrivals)
        return square

    def squares(x):
        x = x * x
        out = x[:, :128]
        for i in range(1, x.shape[1] // 128):
            out = out + x[:, i * 128 : (i + 1) * 128]
        return jnp.sum(out.reshape(-1, 8, 128), axis=0)

    def row_of(x):
        x = jnp.sum(x, axis=0, keepdims=True)
        return x + pltpu.roll(x, 64, 1)

    def step_size(it, square, changes):
        lane = lax.broadcasted_iota(jnp.int32, (1, 128), 1)
        value = jnp.where(lane < 64, row_of(square), row_of(changes))
        for buf, me, devices in (
            (sums_plane, gy * n_ma + ma, plane),
            (sums_line, gx, line),
        ):
            buf[it, me] = value
            mine = buf.at[it, me]
            batch = [send(mine, mine, device) for device in devices]
            if devices is plane:
                yield
            for copy in batch:
                copy.wait_recv()
            value = buf[it, 0]
            for i in range(1, len(devices) + 1):
                value += buf[it, i]
        norm = jnp.sum(jnp.where(lane < 64, value, 0.0), keepdims=True)
        change = jnp.sum(jnp.where(lane < 64, 0.0, value), keepdims=True)
        yield norm / (change + DAMPING * norm)

    intensity = jnp.zeros((kh, n), F32)

    def add_spectra(d, total):
        f = forward(d, 1)
        spec[group_rows(d, 1), :] = f
        return total + folded(f * f)

    other_part = 1 - mine_part
    passed, handed = {}, {}

    def pass_on(d, h):
        ours = piece(d, mine_part, h)
        passed[d, h] = send(ours, ours, gy_next if h < PIECES // 2 else gy_prev)
        handed[d, h] = send(ours, ours, partner)

    def hand_on(d, h):
        theirs = piece(d, other_part, h)
        passed[d, h].wait_recv()
        handed[d, h, 1] = send(theirs, theirs, partner)

    def complete(d):
        for h in range(PIECES):
            handed[d, h].wait_recv()
            handed[d, h, 1].wait_recv()

    arrive(((down, above), (up, below)))
    set_columns(1)
    set_columns(2)
    for h in range(PIECES // 2):
        g = PIECES - 1 - h
        ring[1, h].wait_recv()
        ring[2, h] = send(piece(1, mine_part, h), piece(2, mine_part, h), ma_next)
        pass_on(1, h)
        ring[3, g].wait_recv()
        ring[2, g] = send(piece(3, mine_part, g), piece(2, mine_part, g), ma_prev)
        pass_on(3, g)
    for p in range(2):
        arrive(first_beside[p])
    stacked = [lend(0, p, 0, tx) for p in range(2)]
    for p in range(2):
        keep(0, p)
    for h in range(PIECES // 2):
        g = PIECES - 1 - h
        ring[1, g].wait_recv()
        pass_on(1, g)
        ring[3, h].wait_recv()
        pass_on(3, h)
    for h in range(PIECES // 2):
        g = PIECES - 1 - h
        hand_on(1, h)
        hand_on(3, g)
    for h in range(PIECES // 2):
        g = PIECES - 1 - h
        ring[2, h].wait_recv()
        pass_on(2, h)
        ring[2, g].wait_recv()
        pass_on(2, g)
    for arrivals in stacked:
        arrive(arrivals)
    window(0)
    for h in range(PIECES // 2):
        g = PIECES - 1 - h
        hand_on(1, g)
        hand_on(3, h)
    intensity = add_spectra(0, intensity)
    complete(1)
    intensity = add_spectra(1, intensity)
    for h in range(PIECES):
        hand_on(2, h)
    complete(3)
    intensity = add_spectra(3, intensity)
    complete(2)
    intensity = add_spectra(2, intensity)

    alpha = None
    for it in range(OUTER):
        backward(live * (intensity - meas[...]), alpha)
        square = combine(it)
        window(it + 1)
        last = it + 1 == OUTER

        def group(i, change, last=last):
            rows = group_rows(i * GROUP, GROUP)
            m = forward(i * GROUP, GROUP)
            if not last:
                moved[rows, :] = m
            return change + folded(spec[rows, :] * m)

        zeros = jnp.zeros((kh, n), F32)
        change = 2.0 * lax.fori_loop(0, n_ma // GROUP, group, zeros, unroll=True)
        sums = step_size(it, square, squares(live * change))
        next(sums)
        if not last:

            def power(d, total):
                m = moved[group_rows(d, 1), :]
                return total + folded(m * m)

            moved_power = lax.fori_loop(0, n_ma, power, jnp.zeros((kh, n), F32))
        alpha = next(sums)
        step = alpha * wide[it + 1, :, :, own_cols]
        out_ref[...] = step if it == 0 else out_ref[...] + step
        if not last:
            intensity = intensity + alpha * (change + alpha * moved_power)
    copies.finish()


def solution(mesh):
    sizes = (mesh.shape["gx"], mesh.shape["gy"], mesh.shape["ma"])

    def shards(object_field, probe_modes, measured, positions, slot_counts):
        n = probe_modes.shape[-1]
        _, tx, ty = object_field.shape
        rim, kh = n // 2, n // 2
        height, width = tx + 2 * rim, ty + 2 * rim
        modes = probe_modes.shape[0] * sizes[2]
        row_chunk = tx // CHUNKS
        vmem = pltpu.VMEM
        scratch = [
            pltpu.SMEM(positions.shape, jnp.int32),
            pltpu.SMEM(slot_counts.shape, jnp.int32),
            vmem((2, n, n), BF16),
            vmem((OUTER + 1, 2, tx, width), F32),
            vmem((OUTER + 1, 2, height, n), F32),
            vmem((OUTER + 1, 2, 2, tx, n), F32),
            vmem((sizes[2], 2, 2, n, n), F32),
            vmem((kh, n), F32),
            vmem((n, 2 * n), BF16),
            vmem((2 * n, 2 * n), BF16),
            vmem((2 * n, 2 * n), BF16),
            vmem((2 * n, n), BF16),
            vmem((2, n, n), F32),
            vmem((2 * GROUP, 2 * n, n), BF16),
            vmem((GROUP * n, 2 * n), BF16),
            vmem((modes * kh, 2 * n), F32),
            vmem((modes * kh, 2 * n), F32),
            vmem((2 * GROUP, n, n), BF16),
            vmem((kh, 2 * n), F32),
            vmem((2, n, n), F32),
            vmem((OUTER, 2, height, n), F32),
            vmem((n, 2 * height), BF16),
            vmem((width, 3 * n), BF16),
            vmem((height, 2 * n), BF16),
            vmem((3 * n, width), BF16),
            vmem((3, 8, 128), F32),
            vmem((2 * tx, width), BF16),
            vmem((2 * height, n), BF16),
            vmem((2 * n, n), BF16),
            vmem((2 * row_chunk, 2 * n), BF16),
            vmem((2 * tx, n), BF16),
            vmem((OUTER, 2, tx, width), F32),
            vmem((OUTER, 2, 2, tx, n), F32),
            vmem((OUTER, 2, 2, tx, rim), F32),
            vmem((OUTER, sizes[2] - 1, 2 * CHUNKS, row_chunk // sizes[2], ty), F32),
            vmem((OUTER, sizes[1] * sizes[2], 1, 128), F32),
            vmem((OUTER, sizes[0], 1, 128), F32),
            pltpu.SemaphoreType.REGULAR((5,)),
            pltpu.SemaphoreType.DMA((6,)),
            pltpu.SemaphoreType.DMA((88 + 12 * PIECES + 56 * CHUNKS,)),
            pltpu.SemaphoreType.DMA((88 + 12 * PIECES + 56 * CHUNKS,)),
        ]
        anywhere = pl.BlockSpec(memory_space=pl.ANY)
        in_vmem = pl.BlockSpec(memory_space=pltpu.VMEM)
        update = pl.pallas_call(
            functools.partial(kernel, (*sizes, n, tx, ty)),
            out_shape=pltpu.VMEM(object_field.shape, F32),
            in_specs=[anywhere] * 6,
            out_specs=in_vmem,
            scratch_shapes=scratch,
            compiler_params=pltpu.CompilerParams(
                collective_id=0, has_side_effects=True, vmem_limit_bytes=60 * 1024 * 1024
            ),
        )(object_field, probe_modes, measured, positions, slot_counts, jnp.asarray(dft_parts(n)))
        return object_field + update

    placed = (
        P(None, "gx", "gy"),
        P("ma", None, None, None),
        P("gx", "gy", None, None, None),
        P("gx", "gy", None, None),
        P("gx", "gy"),
    )
    return jax.shard_map(
        shards, mesh=mesh, in_specs=placed, out_specs=P(None, "gx", "gy"), check_vma=False
    )
```
